512 devices in a mesh: dp: 64 (over y, z), mp: 8 (over x, core).
Axes of the slice: x: 4, y: 8, z: 8, core: 2. Of those that a mesh axis runs over, the one named last changes fastest.
Arguments:
- inputs: bfloat16 [64, 2, 256, 2048], P('dp'), may hold values from -6 to 6
- grad_out: bfloat16 [64, 2, 256, 1024], P('dp', None, None, 'mp'), parts along dimension 3, may hold values from -0.5 to 0.5
- momentum: float32 [64, 2048, 1024], P('dp', None, 'mp'), parts along dimension 2, may hold values from -6 to 6
- select: int32 [64, 2, 64, 64], P(None, None, None, 'mp'), parts along dimension 3, may hold values from -1 to 31, as said below
Outputs:
- update: bfloat16 [2048, 1024], P(None, 'mp'), parts along dimension 1
- new_momentum: float32 [64, 2048, 1024], P('dp', None, 'mp'), parts along dimension 2
The draws below stay inside these ranges and needn't reach their ends.
There are 8 independent parts, one for each index of `mp`. The reference program is written for one: setup_inputs(seed, part) draws one part's arguments, and reference() takes and returns one part's arrays. A program takes and returns all parts, laid end to end along the dimension named above; an argument that names none is the same for every part. Nothing has to cross between parts.
Inputs may be any that keep to these rules, and one draw needn't show every extreme that they name: `select`: in each [r, s, o] list the entries that are not -1 are distinct and come first. In every step some owner gets exactly 8 rows from every replica.
All inputs are finite; a program needn't handle non-finite values.
Results may differ from the reference program's by a relative error of at most 0.001.
Values sent between devices are 32-bit elements; how exact they have to be, the bound alone decides.
A program may use at most 64 MiB of HBM per device.

```python
import jax
import jax.numpy as jnp
from jax import lax

ROWS = 2048
COLS = 128
GROUP = 64
TOK = 256
STEPS = 2
CAP = 8
REPLICAS = 64
N_DP = 64


def draw_select(key, part):
    key_tier, key_hot, key_count, key_order = jax.random.split(jax.random.fold_in(key, 7), 4)
    per_owner = ROWS // N_DP
    tier = jax.random.randint(key_tier, (1, STEPS, REPLICAS, 1), 0, 3)
    hottest = jax.random.randint(key_hot, (1, STEPS, 1, 1), 0, REPLICAS)
    drawn = jax.random.randint(key_count, (REPLICAS, STEPS, REPLICAS, 1), 0, CAP + 1)
    counts = jnp.minimum(CAP, drawn * tier // 2)
    owner_ids = lax.broadcasted_iota(jnp.int32, (1, STEPS, REPLICAS, 1), 2)
    counts = jnp.where(owner_ids == hottest, CAP, counts)
    scores = jax.random.randint(key_order, (REPLICAS, STEPS, REPLICAS, per_owner), 0, 1 << 20) * per_owner
    scores = scores + lax.broadcasted_iota(jnp.int32, (REPLICAS, STEPS, REPLICAS, per_owner), 3)
    ordering = jnp.argsort(scores, axis=3)[..., :CAP].astype(jnp.int32)
    slots = lax.broadcasted_iota(jnp.int32, (REPLICAS, STEPS, REPLICAS, CAP), 3)
    return jnp.where(slots < counts, ordering, -1).astype(jnp.int32)


def block_levels(own_key, shape, pieces, low, high):
    def one(axis_at, blocks):
        heights = jax.random.uniform(jax.random.fold_in(jax.random.fold_in(own_key, 6), axis_at), (blocks,), jnp.float32, low / len(pieces), high / len(pieces))
        return jnp.repeat(jnp.exp(heights), shape[axis_at] // blocks).reshape((-1,) + (1,) * (len(shape) - axis_at - 1))

    loudness = one(*pieces[0])
    for cut in pieces[1:]:
        loudness = loudness * one(*cut)
    return loudness


def scatter_about(own_key, dims, width, limit, pieces=(), held_as=jnp.bfloat16):
    values = jax.random.normal(own_key, dims, jnp.float32) * width
    if len(pieces) > 0:
        values = block_levels(own_key, dims, pieces, -0.22, 0.18) * values
    return jnp.clip(values, min=-limit, max=limit).astype(held_as)


def setup_inputs(seed: int = 0, part: int = 0) -> dict:
    arg_keys = jax.random.split(jax.random.key(seed), 5)
    part_keys = jax.random.split(jax.random.fold_in(arg_keys[4], part), 5)
    return {
        "inputs": scatter_about(arg_keys[0], (REPLICAS, STEPS, TOK, ROWS), 1.0, 6.0, ((0, 64),)),
        "grad_out": scatter_about(part_keys[1], (REPLICAS, STEPS, TOK, COLS), 0.0625, 0.5, ((0, 64),)),
        "momentum": scatter_about(part_keys[2], (REPLICAS, ROWS, COLS), 1.0, 6.0, ((0, 64),), jnp.float32),
        "select": draw_select(jax.random.fold_in(jax.random.fold_in(arg_keys[4], part), 71), part),
    }


def dct_matrix(order):
    freq = lax.broadcasted_iota(jnp.int32, (order, order), 0).astype(jnp.float32)
    place = lax.broadcasted_iota(jnp.int32, (order, order), 1).astype(jnp.float32)
    factor = jnp.where(freq == 0.0, jnp.sqrt(1.0 / order), jnp.sqrt(2.0 / order)).astype(jnp.float32)
    return factor * jnp.cos(jnp.pi * (2.0 * place + 1.0) * freq / (2.0 * order))

def forward_blocks(field, dct_table, col_table):
    replicas = field.shape[0]
    shaped = field.reshape(replicas, ROWS // GROUP, GROUP, COLS)
    rowwise = jnp.einsum('ui,raic->rauc', dct_table, shaped, precision=lax.Precision.HIGHEST)
    rowwise = rowwise.reshape(replicas, ROWS, COLS)
    return jnp.einsum('rkc,vc->rkv', rowwise, col_table, precision=lax.Precision.HIGHEST)

def inverse_blocks(coeffs, dct_table, col_table):
    replicas = coeffs.shape[0]
    colwise = jnp.einsum('rkv,vc->rkc', coeffs, col_table, precision=lax.Precision.HIGHEST)
    shaped = colwise.reshape(replicas, ROWS // GROUP, GROUP, COLS)
    back = jnp.einsum('ui,rauc->raic', dct_table, shaped, precision=lax.Precision.HIGHEST)
    return back.reshape(replicas, ROWS, COLS)

def reference(inputs, grad_out, momentum, select):
    dct_table = dct_matrix(GROUP)
    col_table = jnp.kron(jnp.eye(COLS // GROUP, dtype=jnp.float32), dct_table)
    replicas = momentum.shape[0]
    per_owner = ROWS // N_DP
    moment_state = momentum
    update_sum = jnp.zeros((ROWS, COLS), jnp.float32)
    owner_base = (lax.broadcasted_iota(jnp.int32, (replicas, select.shape[2], CAP), 1) * per_owner).astype(jnp.int32)
    replica_rows = lax.broadcasted_iota(jnp.int32, (replicas, select.shape[2] * CAP), 0)
    for iteration in range(STEPS):
        gradient = jnp.einsum('rtk,rtc->rkc', inputs[:, iteration].astype(jnp.float32), grad_out[:, iteration].astype(jnp.float32), precision=lax.Precision.HIGHEST)
        moment_state = 0.999 * moment_state + gradient
        coefficients = forward_blocks(moment_state, dct_table, col_table)
        listed = select[:, iteration]
        global_rows = jnp.where(listed >= 0, listed + owner_base, ROWS).astype(jnp.int32)
        chosen = jnp.zeros((replicas, ROWS + 1), jnp.float32)
        chosen = chosen.at[replica_rows, global_rows.reshape(replicas, -1)].set(1.0)[:, :ROWS]
        sent = coefficients * chosen[:, :, None]
        summed = lax.optimization_barrier(jnp.sum(sent, axis=0))
        update_sum = update_sum + inverse_blocks(summed[None], dct_table, col_table)[0]
        moment_state = moment_state - inverse_blocks(sent, dct_table, col_table)
    return (update_sum.astype(jnp.bfloat16), moment_state)
```

```python
import jax
import jax.numpy as jnp
from jax import lax
from jax.sharding import PartitionSpec as P

GROUP = 64
DECAY = 0.999


def dct_matrix(order):
    freq = lax.broadcasted_iota(jnp.int32, (order, order), 0).astype(jnp.float32)
    place = lax.broadcasted_iota(jnp.int32, (order, order), 1).astype(jnp.float32)
    factor = jnp.where(freq == 0.0, jnp.sqrt(1.0 / order), jnp.sqrt(2.0 / order)).astype(
        jnp.float32
    )
    return factor * jnp.cos(jnp.pi * (2.0 * place + 1.0) * freq / (2.0 * order))


def forward_blocks(field, dct_table, col_table):
    row_count, col_count = field.shape
    order = dct_table.shape[0]
    shaped = field.reshape(row_count // order, order, col_count)
    rowwise = jnp.einsum("ui,aic->auc", dct_table, shaped, precision=lax.Precision.HIGHEST)
    return jnp.dot(
        rowwise.reshape(row_count, col_count), col_table.T, precision=lax.Precision.HIGHEST
    )


def inverse_blocks(coeffs, dct_table, col_table):
    row_count, col_count = coeffs.shape
    order = dct_table.shape[0]
    colwise = jnp.dot(coeffs, col_table, precision=lax.Precision.HIGHEST)
    shaped = colwise.reshape(row_count // order, order, col_count)
    back = jnp.einsum("ui,auc->aic", dct_table, shaped, precision=lax.Precision.HIGHEST)
    return back.reshape(row_count, col_count)


def layer_gradient(inputs, grad_out, iteration):
    return lax.dot_general(
        inputs[0, iteration],
        grad_out[0, iteration],
        (((0,), (0,)), ((), ())),
        preferred_element_type=jnp.float32,
    )


def per_device(inputs, grad_out, momentum, select):
    replica = lax.axis_index("dp")
    owners = lax.axis_size("dp")
    row_count, col_count = momentum.shape[1:]
    per_owner = row_count // owners
    dct_table = dct_matrix(GROUP)
    col_table = jnp.kron(jnp.eye(col_count // GROUP, dtype=jnp.float32), dct_table)
    own_select = lax.dynamic_index_in_dim(select, replica, 0, keepdims=False)
    row_ids = lax.broadcasted_iota(jnp.int32, (1, per_owner, 1), 1)
    kept = None
    sent_total = 0.0
    field = DECAY * momentum[0] + layer_gradient(inputs, grad_out, 0)
    for iteration in range(inputs.shape[1]):
        if iteration:
            field = layer_gradient(inputs, grad_out, iteration)
        coefficients = forward_blocks(field, dct_table, col_table)
        if iteration:
            coefficients = coefficients + DECAY * kept
        listed = own_select[iteration]
        chosen = jnp.any(listed[:, None, :] == row_ids, axis=2)
        chosen = chosen.reshape(row_count, 1)
        sent_total = sent_total + jnp.where(chosen, coefficients, 0.0)
        kept = jnp.where(chosen, 0.0, coefficients)
    summed = lax.psum(sent_total, "dp")
    update = inverse_blocks(summed, dct_table, col_table)
    new_momentum = inverse_blocks(kept, dct_table, col_table)
    return (update.astype(jnp.bfloat16), new_momentum[None])


def solution(mesh):
    return jax.shard_map(
        per_device,
        mesh=mesh,
        in_specs=(
            P("dp", None, None, None),
            P("dp", None, None, "mp"),
            P("dp", None, "mp"),
            P(None, None, None, "mp"),
        ),
        out_specs=(P(None, "mp"), P("dp", None, "mp")),
        check_vma=False,
    )
```

```python
import jax
import jax.numpy as jnp
import numpy as np
from jax import lax
from jax.experimental import pallas as pl
from jax.experimental.pallas import tpu as pltpu
from jax.sharding import PartitionSpec as P

GROUP = 64
DECAY = 0.999
SIDE = 8
PER_OWNER = 32
CAP = 8
STEPS = 2
ROWS = 2048
COLS = 128
TOK = 256
SPAN = 256
BF16 = jnp.bfloat16
F32 = jnp.float32
MESH = pl.DeviceIdType.MESH
FAR_FIRST = (4, 3, 5, 2, 6, 1, 7)


def transform_tables():
    u = np.arange(GROUP)[:, None].astype(np.float64)
    i = np.arange(GROUP)[None, :].astype(np.float64)
    scale = np.where(u == 0, np.sqrt(1.0 / GROUP), np.sqrt(2.0 / GROUP))
    dct = (scale * np.cos(np.pi * (2 * i + 1) * u / (2 * GROUP))).astype(np.float32)
    rows = np.kron(np.eye(SPAN // GROUP, dtype=np.float32), dct)
    cols = np.kron(np.eye(COLS // GROUP, dtype=np.float32), dct)

    def halves(table):
        high = table.astype(BF16)
        low = (table - high.astype(np.float32)).astype(BF16)
        return high, low

    def by_column(table):
        high, low = halves(table)
        zero = np.zeros_like(low)
        return np.concatenate(
            [np.concatenate([high, low], 1), np.concatenate([high, zero], 1)], 0
        )

    def by_row(table):
        return np.concatenate(halves(table), 0)

    return np.concatenate(
        [by_column(cols.T), by_row(rows), by_column(cols), by_row(rows.T)], 0
    )


TABLE_ROWS = 1536


def split(x):
    high = x.astype(BF16)
    low = (x - high.astype(F32)).astype(BF16)
    return jnp.concatenate([high, low], axis=1)


def dot(a, b, dims=(((1,), (0,)), ((), ()))):
    return lax.dot_general(a, b, dims, preferred_element_type=F32)


def folded(x):
    return x[:, :COLS] + x[:, COLS:]


def row_apply(table, x):
    r = dot(table, split(x))
    return r[:SPAN, :COLS] + (r[:SPAN, COLS:] + r[SPAN:, :COLS])


def kernel(
    x_hbm, g_hbm, m_hbm, sel_hbm, tab_hbm,
    upd_ref, mom_ref,
    x_v, g_v, m_v, sel_v, tab_v, h_v, f_v, c_v, kept_v,
    zsend, ysend, zin, yin, pz, py, p2in, tout, u_v,
    load_sem, r1s, r1r, p2s, p2r, a1s, a1r, a2s, a2r,
):
    me = lax.axis_index("dp")
    mp = lax.axis_index("mp")
    y = me // SIDE
    z = me % SIDE
    par = (y + z) % 2

    def at(yy, zz):
        return (yy * SIDE + zz, mp)

    loads = []

    def load(src, dst):
        copy = pltpu.make_async_copy(src, dst, load_sem.at[len(loads)])
        copy.start()
        loads.append(copy)
        return copy

    load_g = load(g_hbm.at[0], g_v)
    load_tab = load(tab_hbm.at[pl.ds(0, 768)], tab_v.at[pl.ds(0, 768)])
    load_x0 = load(x_hbm.at[0, 0], x_v.at[0])
    load_m = load(m_hbm.at[0], m_v)
    load_sel = load(sel_hbm, sel_v)
    load_x1 = load(x_hbm.at[0, 1], x_v.at[1])
    load_tab2 = load(tab_hbm.at[pl.ds(768, 768)], tab_v.at[pl.ds(768, 768)])

    barrier = pltpu.get_barrier_semaphore()
    for d in range(1, SIDE):
        pl.semaphore_signal(barrier, inc=1, device_id=at((y + d) % SIDE, z), device_id_type=MESH)
        pl.semaphore_signal(barrier, inc=1, device_id=at(y, (z + d) % SIDE), device_id_type=MESH)

    load_g.wait()
    load_tab.wait()
    for s in range(STEPS):
        h_v[s] = split(folded(dot(g_v[s], tab_v[0:COLS, :])))

    tn = (((0,), (0,)), ((), ()))
    load_x0.wait()
    load_m.wait()
    for g in range(SIDE):
        rows = pl.ds(g * SPAN, SPAN)
        grad = folded(dot(x_v[0, :, rows], h_v[0], tn))
        carried = folded(dot(split(m_v[rows, :]), tab_v[0:SPAN, :]))
        f_v[0, g] = DECAY * carried + grad
    load_x1.wait()
    for g in range(SIDE):
        rows = pl.ds(g * SPAN, SPAN)
        f_v[1, g] = folded(dot(x_v[1, :, rows], h_v[1], tn))

    load_sel.wait()
    lane = lax.broadcasted_iota(jnp.int32, (CAP, SPAN), 1)
    ones = jnp.ones((SIDE * CAP, COLS), BF16)
    owner_lane = lax.broadcasted_iota(jnp.int32, (CAP, SIDE * SIDE), 1)
    forward = tab_v[256:768, :]
    for s in range(STEPS):
        own = sel_v[me, s]
        own = jnp.where(own >= 0, own + (owner_lane % SIDE) * PER_OWNER, -1)
        for g in range(SIDE):
            c = row_apply(forward, f_v[s, g])
            if s:
                c = c + DECAY * kept_v[g]
            picks = [
                (own[:, g * SIDE + q : g * SIDE + q + 1] == lane).astype(F32)
                for q in range(SIDE)
            ]
            onehot = jnp.concatenate(picks, axis=0).astype(BF16)
            mask = dot(onehot, ones, tn)
            packed = folded(dot(onehot, split(c)))
            kept_v[g] = jnp.where(mask > 0.5, 0.0, c)
            for q in range(SIDE):
                tile = packed[q * CAP : (q + 1) * CAP]
                if (g + q) % 2 == 0:
                    zsend[q, g // 2, s * CAP : (s + 1) * CAP, :] = tile
                else:
                    ysend[g, q // 2, s * CAP : (s + 1) * CAP, :] = tile

    pl.semaphore_wait(barrier, 2 * (SIDE - 1))

    def first(axis, d):
        if axis == 0:
            to = (z + d) % SIDE
            return pltpu.make_async_remote_copy(
                src_ref=zsend.at[to], dst_ref=zin.at[z],
                send_sem=r1s.at[0, d], recv_sem=r1r.at[0, d],
                device_id=at(y, to), device_id_type=MESH,
            )
        to = (y + d) % SIDE
        return pltpu.make_async_remote_copy(
            src_ref=ysend.at[to], dst_ref=yin.at[y],
            send_sem=r1s.at[1, d], recv_sem=r1r.at[1, d],
            device_id=at(to, z), device_id_type=MESH,
        )

    for d in FAR_FIRST:
        for axis in range(2):
            first(axis, d).start()
    zin[z] = zsend[z]
    yin[y] = ysend[y]

    load_tab2.wait()
    pick_row = lax.broadcasted_iota(jnp.int32, (COLS, SIDE * SIDE), 0)
    pick_lane = lax.broadcasted_iota(jnp.int32, (COLS, SIDE * SIDE), 1)
    place = (lax.broadcasted_iota(jnp.int32, (COLS, COLS), 0) % PER_OWNER).astype(F32)
    nt = (((1,), (1,)), ((), ()))

    def scatter_table(listed, owner):
        chooser = (pick_lane == owner).astype(F32).astype(BF16)
        wanted = dot(chooser, listed.astype(F32).astype(BF16), nt)
        return (wanted == place).astype(F32).astype(BF16)

    along_z = sel_v[pl.ds(y * SIDE, SIDE)].reshape(COLS, SIDE * SIDE)
    along_y = jnp.concatenate(
        [sel_v[q * SIDE + z].reshape(STEPS * CAP, SIDE * SIDE) for q in range(SIDE)], axis=0
    )
    index = pick_row // PER_OWNER
    table_z = scatter_table(along_z, (2 * index + z % 2) * SIDE + z)
    table_y = scatter_table(along_y, y * SIDE + 2 * index + (y + 1) % 2)

    by_col = tab_v[768:1024, :]
    backward = tab_v[1024:1536, :]
    for g in range(SIDE):
        f_v[0, g] = folded(dot(split(kept_v[g]), by_col))
    for g in range(SIDE):
        mom_ref[g * SPAN : (g + 1) * SPAN, :] = row_apply(backward, f_v[0, g])

    for d in FAR_FIRST:
        for axis in range(2):
            first(axis, d).wait_recv()
    for i in range(4):
        block = slice(i * PER_OWNER, (i + 1) * PER_OWNER)
        pz[i] = folded(dot(table_z[block], split(zin[:, i].reshape(COLS, COLS))))
        py[i] = folded(dot(table_y[block], split(yin[:, i].reshape(COLS, COLS))))

    def second(axis, i):
        if axis == 0:
            to = 2 * i + z % 2
            return to != y, pltpu.make_async_remote_copy(
                src_ref=pz.at[i], dst_ref=p2in.at[y],
                send_sem=p2s.at[0, i], recv_sem=p2r.at[y],
                device_id=at(to, z), device_id_type=MESH,
            )
        to = 2 * i + (y + 1) % 2
        return to != z, pltpu.make_async_remote_copy(
            src_ref=py.at[i], dst_ref=p2in.at[z],
            send_sem=p2s.at[1, i], recv_sem=p2r.at[z],
            device_id=at(y, to), device_id_type=MESH,
        )

    for i in range(4):
        for axis in range(2):
            other, copy = second(axis, i)

            @pl.when(other)
            def _():
                copy.start()

            @pl.when(jnp.logical_not(other))
            def _():
                if axis == 0:
                    p2in[y] = pz[i]
                else:
                    p2in[z] = py[i]

    slot = y + par * (z - y)
    for k in range(SIDE):

        @pl.when(k != slot)
        def _():
            pltpu.make_async_remote_copy(
                src_ref=pz.at[0], dst_ref=p2in.at[k],
                send_sem=p2s.at[0, 0], recv_sem=p2r.at[k],
                device_id=at((y + 1) % SIDE, z), device_id_type=MESH,
            ).wait_recv()

    total = p2in[0]
    for k in range(1, SIDE):
        total = total + p2in[k]
    line = z + par * (y - z)
    mine = (y + par * (z - y)) // 2
    final = folded(dot(split(total), by_col))
    tout[...] = final
    u_v[par, line, mine] = final

    def third(d):
        to_y = (y + (1 - par) * d) % SIDE
        to_z = (z + par * d) % SIDE
        return pltpu.make_async_remote_copy(
            src_ref=tout, dst_ref=u_v.at[par, line, mine],
            send_sem=a1s.at[d], recv_sem=a1r.at[par, mine],
            device_id=at(to_y, to_z), device_id_type=MESH,
        )

    for d in FAR_FIRST:
        third(d).start()

    def third_arrived(axis, i):
        where = z if axis == 0 else y
        own = (par == axis) & (mine == i)

        @pl.when(jnp.logical_not(own))
        def _():
            pltpu.make_async_remote_copy(
                src_ref=tout, dst_ref=u_v.at[axis, where, i],
                send_sem=a1s.at[1], recv_sem=a1r.at[axis, i],
                device_id=at((y + 1) % SIDE, z), device_id_type=MESH,
            ).wait_recv()

    def relay(axis, way, level, half):
        pos = z if axis == 0 else y
        step = 1 if way == 0 else SIDE - 1
        source = (pos + (level - 1) * (SIDE - step)) % SIDE
        to = (pos + step) % SIDE
        block = u_v.at[axis, source, pl.ds(half * 2, 2)]
        return pltpu.make_async_remote_copy(
            src_ref=block, dst_ref=block,
            send_sem=a2s.at[axis, way, level - 1, half],
            recv_sem=a2r.at[axis, way, level - 1, half],
            device_id=at(y, to) if axis == 0 else at(to, z), device_id_type=MESH,
        )

    def relay_arrived(axis, way, level, half):
        pos = z if axis == 0 else y
        step = 1 if way == 0 else SIDE - 1
        source = (pos + level * (SIDE - step)) % SIDE
        block = u_v.at[axis, source, pl.ds(half * 2, 2)]
        pltpu.make_async_remote_copy(
            src_ref=block, dst_ref=block,
            send_sem=a2s.at[axis, way, level - 1, half],
            recv_sem=a2r.at[axis, way, level - 1, half],
            device_id=at((y + 1) % SIDE, z), device_id_type=MESH,
        ).wait_recv()

    def levels(way, half):
        return 4 if way == half else 3

    sent = []
    for half in range(2):
        for axis in range(2):
            for i in (2 * half, 2 * half + 1):
                third_arrived(axis, i)
            for way in range(2):
                copy = relay(axis, way, 1, half)
                copy.start()
                sent.append(copy)
    for level in range(1, 5):
        for half in range(2):
            for axis in range(2):
                for way in range(2):
                    if level <= levels(way, half):
                        relay_arrived(axis, way, level, half)
                        if level < levels(way, half):
                            copy = relay(axis, way, level + 1, half)
                            copy.start()
                            sent.append(copy)

    for g in range(SIDE):
        parts = [
            u_v[0, q, g // 2] if (g + q) % 2 == 0 else u_v[1, g, q // 2] for q in range(SIDE)
        ]
        block = row_apply(backward, jnp.concatenate(parts, axis=0))
        upd_ref[g * SPAN : (g + 1) * SPAN, :] = block.astype(BF16)

    for d in FAR_FIRST:
        for axis in range(2):
            first(axis, d).wait_send()
    for i in range(4):
        for axis in range(2):
            other, copy = second(axis, i)

            @pl.when(other)
            def _():
                copy.wait_send()

    for d in FAR_FIRST:
        third(d).wait_send()
    for copy in sent:
        copy.wait_send()


def per_device(inputs, grad_out, momentum, select):
    table = jnp.asarray(transform_tables())
    listed = jnp.transpose(select, (0, 1, 3, 2))
    hbm = pl.BlockSpec(memory_space=pl.ANY)
    vmem = pl.BlockSpec(memory_space=pltpu.VMEM)
    update, new_momentum = pl.pallas_call(
        kernel,
        out_shape=(
            jax.ShapeDtypeStruct((ROWS, COLS), BF16),
            jax.ShapeDtypeStruct((ROWS, COLS), F32),
        ),
        in_specs=[hbm] * 5,
        out_specs=(vmem, vmem),
        scratch_shapes=[
            pltpu.VMEM((STEPS, TOK, ROWS), BF16),
            pltpu.VMEM((STEPS, TOK, COLS), BF16),
            pltpu.VMEM((ROWS, COLS), F32),
            pltpu.VMEM((SIDE * SIDE, STEPS, CAP, SIDE * SIDE), jnp.int32),
            pltpu.VMEM((TABLE_ROWS, SPAN), BF16),
            pltpu.VMEM((STEPS, TOK, 2 * COLS), BF16),
            pltpu.VMEM((STEPS, SIDE, SPAN, COLS), F32),
            pltpu.VMEM((8, COLS), F32),
            pltpu.VMEM((SIDE, SPAN, COLS), F32),
            pltpu.VMEM((SIDE, 4, STEPS * CAP, COLS), F32),
            pltpu.VMEM((SIDE, 4, STEPS * CAP, COLS), F32),
            pltpu.VMEM((SIDE, 4, STEPS * CAP, COLS), F32),
            pltpu.VMEM((SIDE, 4, STEPS * CAP, COLS), F32),
            pltpu.VMEM((4, PER_OWNER, COLS), F32),
            pltpu.VMEM((4, PER_OWNER, COLS), F32),
            pltpu.VMEM((SIDE, PER_OWNER, COLS), F32),
            pltpu.VMEM((PER_OWNER, COLS), F32),
            pltpu.VMEM((2, SIDE, 4, PER_OWNER, COLS), F32),
            pltpu.SemaphoreType.DMA((7,)),
            pltpu.SemaphoreType.DMA((2, SIDE)),
            pltpu.SemaphoreType.DMA((2, SIDE)),
            pltpu.SemaphoreType.DMA((2, 4)),
            pltpu.SemaphoreType.DMA((SIDE,)),
            pltpu.SemaphoreType.DMA((SIDE,)),
            pltpu.SemaphoreType.DMA((2, 4)),
            pltpu.SemaphoreType.DMA((2, 2, 4, 2)),
            pltpu.SemaphoreType.DMA((2, 2, 4, 2)),
        ],
        compiler_params=pltpu.CompilerParams(
            collective_id=0, has_side_effects=True, vmem_limit_bytes=62 << 20
        ),
    )(inputs, grad_out, momentum, listed, table)
    return (update, new_momentum[None])


def solution(mesh):
    return jax.shard_map(
        per_device,
        mesh=mesh,
        in_specs=(
            P("dp", None, None, None),
            P("dp", None, None, "mp"),
            P("dp", None, "mp"),
            P(None, None, None, "mp"),
        ),
        out_specs=(P(None, "mp"), P("dp", None, "mp")),
        check_vma=False,
    )
```

```python
import jax
import jax.numpy as jnp
import numpy as np
from jax import lax
from jax.experimental import pallas as pl
from jax.experimental.pallas import tpu as pltpu
from jax.sharding import PartitionSpec as P

GROUP = 64
DECAY = 0.999
SIDE = 8
PER_OWNER = 32
CAP = 8
STEPS = 2
ROWS = 2048
COLS = 128
TOK = 256
SPAN = 256
BF16 = jnp.bfloat16
F32 = jnp.float32
MESH = pl.DeviceIdType.MESH
FAR_FIRST = (4, 3, 5, 2, 6, 1, 7)
NEAR_EVEN = (0, 2, -2, 4)
NEAR_ODD = (1, -1, 3, -3)


def transform_tables():
    u = np.arange(GROUP)[:, None].astype(np.float64)
    i = np.arange(GROUP)[None, :].astype(np.float64)
    scale = np.where(u == 0, np.sqrt(1.0 / GROUP), np.sqrt(2.0 / GROUP))
    dct = (scale * np.cos(np.pi * (2 * i + 1) * u / (2 * GROUP))).astype(np.float32)
    rows = np.kron(np.eye(SPAN // GROUP, dtype=np.float32), dct)

    def by_row(table):
        high = table.astype(BF16)
        low = (table - high.astype(np.float32)).astype(BF16)
        return np.concatenate([high, low], 0)

    return np.concatenate([by_row(rows), by_row(rows.T)], 0)


TABLE_ROWS = 1024


def split(x):
    high = x.astype(BF16)
    low = (x - high.astype(F32)).astype(BF16)
    return jnp.concatenate([high, low], axis=1)


def dot(a, b, dims=(((1,), (0,)), ((), ()))):
    return lax.dot_general(a, b, dims, preferred_element_type=F32)


def folded(x):
    return x[:, :COLS] + x[:, COLS:]


def row_apply(table, x):
    r = dot(table, split(x))
    return r[:SPAN, :COLS] + (r[:SPAN, COLS:] + r[SPAN:, :COLS])


def kernel(
    x_hbm, g_hbm, m_hbm, sel_hbm, tab_hbm,
    upd_ref, mom_ref,
    x_v, g_v, m_v, sel_v, tab_v, f_v, kept_v,
    zsend, ysend, zin, yin, pz, py, p2in, tout, u_v,
    load_sem, r1s, r1r, p2s, p2r, a1s, a1r, a2s, a2r,
):
    me = lax.axis_index("dp")
    mp = lax.axis_index("mp")
    y = me // SIDE
    z = me % SIDE
    par = (y + z) % 2

    def at(yy, zz):
        return (yy * SIDE + zz, mp)

    loads = []

    def load(src, dst):
        copy = pltpu.make_async_copy(src, dst, load_sem.at[len(loads)])
        copy.start()
        loads.append(copy)
        return copy

    load_g = load(g_hbm.at[0], g_v)
    load_tab = load(tab_hbm.at[pl.ds(0, 512)], tab_v.at[pl.ds(0, 512)])
    load_x0 = load(x_hbm.at[0, 0], x_v.at[0])
    load_m = load(m_hbm.at[0], m_v)
    load_sel = load(sel_hbm, sel_v)
    load_x1 = load(x_hbm.at[0, 1], x_v.at[1])
    load_tab2 = load(tab_hbm.at[pl.ds(512, 512)], tab_v.at[pl.ds(512, 512)])

    barrier = pltpu.get_barrier_semaphore()
    for d in range(1, SIDE):
        pl.semaphore_signal(barrier, inc=1, device_id=at((y + d) % SIDE, z), device_id_type=MESH)
        pl.semaphore_signal(barrier, inc=1, device_id=at(y, (z + d) % SIDE), device_id_type=MESH)

    tn = (((0,), (0,)), ((), ()))
    load_g.wait()
    load_x0.wait()
    load_m.wait()
    for g in range(SIDE):
        rows = pl.ds(g * SPAN, SPAN)
        f_v[0, g] = DECAY * m_v[rows, :] + dot(x_v[0, :, rows], g_v[0], tn)
    load_x1.wait()
    for g in range(SIDE):
        rows = pl.ds(g * SPAN, SPAN)
        f_v[1, g] = dot(x_v[1, :, rows], g_v[1], tn)

    load_tab.wait()
    load_sel.wait()
    lane = lax.broadcasted_iota(jnp.int32, (CAP, SPAN), 1)
    ones = jnp.ones((SIDE * CAP, COLS), BF16)
    owner_lane = lax.broadcasted_iota(jnp.int32, (CAP, SIDE * SIDE), 1)
    forward = tab_v[0:512, :]
    for s in range(STEPS):
        own = sel_v[me, s]
        own = jnp.where(own >= 0, own + (owner_lane % SIDE) * PER_OWNER, -1)
        for g in range(SIDE):
            c = row_apply(forward, f_v[s, g])
            if s:
                c = c + DECAY * kept_v[g]
            picks = [
                (own[:, g * SIDE + q : g * SIDE + q + 1] == lane).astype(F32)
                for q in range(SIDE)
            ]
            onehot = jnp.concatenate(picks, axis=0).astype(BF16)
            mask = dot(onehot, ones, tn)
            packed = folded(dot(onehot, split(c)))
            kept_v[g] = jnp.where(mask > 0.5, 0.0, c)
            for q in range(SIDE):
                tile = packed[q * CAP : (q + 1) * CAP]
                if (g + q) % 2 == 0:
                    zsend[q, g // 2, s * CAP : (s + 1) * CAP, :] = tile
                else:
                    ysend[g, q // 2, s * CAP : (s + 1) * CAP, :] = tile

    pl.semaphore_wait(barrier, 2 * (SIDE - 1))
    def first(axis, d):
        if axis == 0:
            to = (z + d) % SIDE
            return pltpu.make_async_remote_copy(
                src_ref=zsend.at[to], dst_ref=zin.at[z],
                send_sem=r1s.at[0, d], recv_sem=r1r.at[0, d],
                device_id=at(y, to), device_id_type=MESH,
            )
        to = (y + d) % SIDE
        return pltpu.make_async_remote_copy(
            src_ref=ysend.at[to], dst_ref=yin.at[y],
            send_sem=r1s.at[1, d], recv_sem=r1r.at[1, d],
            device_id=at(to, z), device_id_type=MESH,
        )

    for d in FAR_FIRST:
        for axis in range(2):
            first(axis, d).start()
    zin[z] = zsend[z]
    yin[y] = ysend[y]

    load_tab2.wait()
    pick_row = lax.broadcasted_iota(jnp.int32, (COLS, SIDE * SIDE), 0)
    pick_lane = lax.broadcasted_iota(jnp.int32, (COLS, SIDE * SIDE), 1)
    place = (lax.broadcasted_iota(jnp.int32, (COLS, COLS), 0) % PER_OWNER).astype(F32)
    nt = (((1,), (1,)), ((), ()))

    def scatter_table(listed, owner):
        chooser = (pick_lane == owner).astype(F32).astype(BF16)
        wanted = dot(chooser, listed.astype(F32).astype(BF16), nt)
        return (wanted == place).astype(F32).astype(BF16)

    along_z = sel_v[pl.ds(y * SIDE, SIDE)].reshape(COLS, SIDE * SIDE)
    along_y = jnp.concatenate(
        [sel_v[q * SIDE + z].reshape(STEPS * CAP, SIDE * SIDE) for q in range(SIDE)], axis=0
    )
    index = pick_row // PER_OWNER
    table_z = scatter_table(along_z, (2 * index + z % 2) * SIDE + z)
    table_y = scatter_table(along_y, y * SIDE + 2 * index + (y + 1) % 2)

    backward = tab_v[512:1024, :]
    for g in range(SIDE):
        mom_ref[g * SPAN : (g + 1) * SPAN, :] = row_apply(backward, kept_v[g])

    for d in FAR_FIRST:
        for axis in range(2):
            first(axis, d).wait_recv()
    for i in range(4):
        block = slice(i * PER_OWNER, (i + 1) * PER_OWNER)
        pz[i] = folded(dot(table_z[block], split(zin[:, i].reshape(COLS, COLS))))
        py[i] = folded(dot(table_y[block], split(yin[:, i].reshape(COLS, COLS))))

    def done1():
        for d in FAR_FIRST:
            for axis in range(2):
                first(axis, d).wait_send()
    def peer(axis, k):
        far = par if axis == 0 else 1 - par
        offset = NEAR_EVEN[k] + far * (NEAR_ODD[k] - NEAR_EVEN[k])
        return far, ((y if axis == 0 else z) + offset + SIDE) % SIDE

    def second(axis, k):
        _, to = peer(axis, k)
        return pltpu.make_async_remote_copy(
            src_ref=(pz if axis == 0 else py).at[to // 2],
            dst_ref=p2in.at[y if axis == 0 else z],
            send_sem=p2s.at[axis, k], recv_sem=p2r.at[y if axis == 0 else z],
            device_id=at(to, z) if axis == 0 else at(y, to), device_id_type=MESH,
        )

    for k in (3, 2, 1):
        for axis in range(2):
            second(axis, k).start()
    along = y + par * (z - y)
    line = z + par * (y - z)
    mine = along // 2
    for axis in range(2):
        far, _ = peer(axis, 0)

        @pl.when(far == 1)
        def _():
            second(axis, 0).start()

        @pl.when(far == 0)
        def _():
            p2in[along] = (pz if axis == 0 else py)[mine]

    total = p2in[along]
    for d in (1, 7, 2, 6, 3, 5, 4):
        source = (along + d) % SIDE
        pltpu.make_async_remote_copy(
            src_ref=pz.at[0], dst_ref=p2in.at[source],
            send_sem=p2s.at[0, 0], recv_sem=p2r.at[source],
            device_id=at((y + 1) % SIDE, z), device_id_type=MESH,
        ).wait_recv()
        total = total + p2in[source]
    tout[...] = total
    u_v[par, line, mine] = total

    def done2():
        done1()
        for axis in range(2):
            for k in (3, 2, 1):
                second(axis, k).wait_send()
            far, _ = peer(axis, 0)

            @pl.when(far == 1)
            def _():
                second(axis, 0).wait_send()

    def third(d):
        to_y = (y + (1 - par) * d) % SIDE
        to_z = (z + par * d) % SIDE
        return pltpu.make_async_remote_copy(
            src_ref=tout, dst_ref=u_v.at[par, line, mine],
            send_sem=a1s.at[d], recv_sem=a1r.at[par, mine],
            device_id=at(to_y, to_z), device_id_type=MESH,
        )

    for d in FAR_FIRST:
        third(d).start()

    def third_arrived(axis, k):
        far, source = peer(axis, k)
        where = z if axis == 0 else y

        def wait():
            pltpu.make_async_remote_copy(
                src_ref=tout, dst_ref=u_v.at[axis, where, source // 2],
                send_sem=a1s.at[1], recv_sem=a1r.at[axis, source // 2],
                device_id=at((y + 1) % SIDE, z), device_id_type=MESH,
            ).wait_recv()

        if k:
            wait()
        else:
            pl.when(far == 1)(wait)
        return source // 2

    def spread(axis, way, hop, behind, i):
        pos = z if axis == 0 else y
        step = 1 if way == 0 else SIDE - 1
        source = (pos + behind * (SIDE - step)) % SIDE
        to = (pos + hop * step) % SIDE
        block = u_v.at[axis, source, i]
        slot = 2 * (behind + hop - 1) + way
        return pltpu.make_async_remote_copy(
            src_ref=block, dst_ref=block,
            send_sem=a2s.at[axis, slot, i], recv_sem=a2r.at[axis, slot, i],
            device_id=at(y, to) if axis == 0 else at(to, z), device_id_type=MESH,
        )

    def spread_arrived(axis, way, distance, i):
        pos = z if axis == 0 else y
        step = 1 if way == 0 else SIDE - 1
        source = (pos + distance * (SIDE - step)) % SIDE
        block = u_v.at[axis, source, i]
        slot = 2 * (distance - 1) + way
        pltpu.make_async_remote_copy(
            src_ref=block, dst_ref=block,
            send_sem=a2s.at[axis, slot, i], recv_sem=a2r.at[axis, slot, i],
            device_id=at((y + 1) % SIDE, z), device_id_type=MESH,
        ).wait_recv()

    order = {}
    for k in range(4):
        for axis in range(2):
            i = third_arrived(axis, k)
            order[axis, k] = i
            for way in range(2):
                spread(axis, way, 2, 0, i).start()
    for k in range(4):
        for axis in range(2):
            for way in range(2):
                spread(axis, way, 1, 0, order[axis, k]).start()
    for k in range(4):
        for axis in range(2):
            i = order[axis, k]
            for way in range(2):
                spread_arrived(axis, way, 2, i)

                @pl.when(i // 2 == way)
                def _():
                    spread(axis, way, 2, 2, i).start()

                spread(axis, way, 1, 2, i).start()
    for axis in range(2):
        for way in range(2):
            for i in range(4):
                spread_arrived(axis, way, 1, i)
    for axis in range(2):
        for way in range(2):
            for i in range(4):
                spread_arrived(axis, way, 3, i)
                if i // 2 == way:
                    spread_arrived(axis, way, 4, i)

    for g in range(SIDE):
        parts = [
            u_v[0, q, g // 2] if (g + q) % 2 == 0 else u_v[1, g, q // 2] for q in range(SIDE)
        ]
        block = row_apply(backward, jnp.concatenate(parts, axis=0))
        upd_ref[g * SPAN : (g + 1) * SPAN, :] = block.astype(BF16)

    done2()
    for d in FAR_FIRST:
        third(d).wait_send()
    for axis in range(2):
        for way in range(2):
            for i in range(4):
                spread(axis, way, 2, 0, i).wait_send()
                spread(axis, way, 1, 0, i).wait_send()
                spread(axis, way, 1, 2, i).wait_send()
                if i // 2 == way:
                    spread(axis, way, 2, 2, i).wait_send()


def deliver(upd_ref, mom_ref, upd_out, mom_out, sem):
    first = pltpu.make_async_copy(mom_ref, mom_out, sem.at[0])
    second = pltpu.make_async_copy(upd_ref, upd_out, sem.at[1])
    first.start()
    second.start()
    first.wait()
    second.wait()


def per_device(inputs, grad_out, momentum, select):
    table = jnp.asarray(transform_tables())
    listed = jnp.transpose(select, (0, 1, 3, 2))
    hbm = pl.BlockSpec(memory_space=pl.ANY)
    vmem = pl.BlockSpec(memory_space=pltpu.VMEM)
    operands = [
        pltpu.with_memory_space_constraint(v, pltpu.HBM)
        for v in (inputs, grad_out, momentum, listed, table)
    ]
    outs = (
        jax.ShapeDtypeStruct((ROWS, COLS), BF16),
        jax.ShapeDtypeStruct((ROWS, COLS), F32),
    )
    update, new_momentum = pl.pallas_call(
        kernel,
        out_shape=outs,
        in_specs=[hbm] * 5,
        out_specs=(vmem, vmem),
        scratch_shapes=[
            pltpu.VMEM((STEPS, TOK, ROWS), BF16),
            pltpu.VMEM((STEPS, TOK, COLS), BF16),
            pltpu.VMEM((ROWS, COLS), F32),
            pltpu.VMEM((SIDE * SIDE, STEPS, CAP, SIDE * SIDE), jnp.int32),
            pltpu.VMEM((TABLE_ROWS, SPAN), BF16),
            pltpu.VMEM((STEPS, SIDE, SPAN, COLS), F32),
            pltpu.VMEM((SIDE, SPAN, COLS), F32),
            pltpu.VMEM((SIDE, 4, STEPS * CAP, COLS), F32),
            pltpu.VMEM((SIDE, 4, STEPS * CAP, COLS), F32),
            pltpu.VMEM((SIDE, 4, STEPS * CAP, COLS), F32),
            pltpu.VMEM((SIDE, 4, STEPS * CAP, COLS), F32),
            pltpu.VMEM((4, PER_OWNER, COLS), F32),
            pltpu.VMEM((4, PER_OWNER, COLS), F32),
            pltpu.VMEM((SIDE, PER_OWNER, COLS), F32),
            pltpu.VMEM((PER_OWNER, COLS), F32),
            pltpu.VMEM((2, SIDE, 4, PER_OWNER, COLS), F32),
            pltpu.SemaphoreType.DMA((7,)),
            pltpu.SemaphoreType.DMA((2, SIDE)),
            pltpu.SemaphoreType.DMA((2, SIDE)),
            pltpu.SemaphoreType.DMA((2, 4)),
            pltpu.SemaphoreType.DMA((SIDE,)),
            pltpu.SemaphoreType.DMA((SIDE,)),
            pltpu.SemaphoreType.DMA((2, 4)),
            pltpu.SemaphoreType.DMA((2, 8, 4)),
            pltpu.SemaphoreType.DMA((2, 8, 4)),
        ],
        compiler_params=pltpu.CompilerParams(
            collective_id=0, has_side_effects=True, vmem_limit_bytes=40 << 20
        ),
    )(*operands)
    update, new_momentum = pl.pallas_call(
        deliver,
        out_shape=outs,
        in_specs=[hbm] * 2,
        out_specs=(hbm, hbm),
        scratch_shapes=[pltpu.SemaphoreType.DMA((2,))],
        compiler_params=pltpu.CompilerParams(vmem_limit_bytes=8 << 20),
    )(update, new_momentum)
    return (update, new_momentum[None])


def solution(mesh):
    return jax.shard_map(
        per_device,
        mesh=mesh,
        in_specs=(
            P("dp", None, None, None),
            P("dp", None, None, "mp"),
            P("dp", None, "mp"),
            P(None, None, None, "mp"),
        ),
        out_specs=(P(None, "mp"), P("dp", None, "mp")),
        check_vma=False,
    )
```

```python
import jax
import jax.numpy as jnp
import numpy as np
from jax import lax
from jax.experimental import pallas as pl
from jax.experimental.pallas import tpu as pltpu
from jax.sharding import PartitionSpec as P

GROUP = 64
DECAY = 0.999
SIDE = 8
PER_OWNER = 32
CAP = 8
STEPS = 2
ROWS = 2048
COLS = 128
TOK = 256
SPAN = 256
BF16 = jnp.bfloat16
F32 = jnp.float32
MESH = pl.DeviceIdType.MESH
FAR_FIRST = (4, 3, 5, 2, 6, 1, 7)
NEAR_EVEN = (0, 2, -2, 4)
NEAR_ODD = (1, -1, 3, -3)


def transform_tables():
    u = np.arange(GROUP)[:, None].astype(np.float64)
    i = np.arange(GROUP)[None, :].astype(np.float64)
    scale = np.where(u == 0, np.sqrt(1.0 / GROUP), np.sqrt(2.0 / GROUP))
    dct = (scale * np.cos(np.pi * (2 * i + 1) * u / (2 * GROUP))).astype(np.float32)

    def parts(table):
        high = table.astype(BF16)
        low = (table - high.astype(np.float32)).astype(BF16)
        return np.concatenate([high, high, low, low], 1)

    return np.concatenate([parts(dct), parts(dct.T)], 0)


def split(x):
    high = x.astype(BF16)
    low = (x - high.astype(F32)).astype(BF16)
    return jnp.concatenate([high, low], axis=1)


def dot(a, b, dims=(((1,), (0,)), ((), ()))):
    return lax.dot_general(a, b, dims, preferred_element_type=F32)


def folded(x):
    return x[:, :COLS] + x[:, COLS:]


def blocks_apply(table, x):
    high = x.astype(BF16)
    low = (x - high.astype(F32)).astype(BF16)

    def stacked(b):
        rows = slice(b * GROUP, (b + 1) * GROUP)
        return jnp.concatenate([high[rows], low[rows]], axis=0)

    out = []
    for b in range(0, SPAN // GROUP, 2):
        pair = jnp.concatenate([stacked(b), stacked(b + 1)], axis=1)
        r = dot(table, jnp.concatenate([pair, pair], axis=0))
        out += [r[:, :COLS], r[:, COLS:]]
    return jnp.concatenate(out, axis=0)


CHUNKS = 2
HALVES = 2
PER_CHUNK = 4 // CHUNKS


def kernel(
    x_hbm, g_hbm, m_hbm, sel_hbm, tab_hbm,
    u_v, mom_ref, back_v,
    x_v, g_v, m_v, sel_v, own_v, tab_v, f_v, kept_v, pick_v, keep_v,
    zsend, ysend, zin, yin, pz, py, p2in, tout,
    load_sem, r1s, r1r, p2s, p2r, a1s, a1r, a2s, a2r,
):
    me = lax.axis_index("dp")
    mp = lax.axis_index("mp")
    y = me // SIDE
    z = me % SIDE
    par = (y + z) % 2

    def at(yy, zz):
        return (yy * SIDE + zz, mp)

    loads = []

    def load(src, dst):
        copy = pltpu.make_async_copy(src, dst, load_sem.at[len(loads)])
        copy.start()
        loads.append(copy)
        return copy

    half_rows = ROWS // HALVES
    load_own = load(sel_hbm.at[me], own_v)
    load_g = load(g_hbm.at[0], g_v)
    load_tab = load(tab_hbm.at[pl.ds(0, GROUP)], tab_v)
    load_half = []
    for half in range(HALVES):
        rows = pl.ds(half * half_rows, half_rows)
        load_half.append(
            [
                load(x_hbm.at[0, 0, :, rows], x_v.at[0, :, rows]),
                load(m_hbm.at[0, rows], m_v.at[rows]),
                load(x_hbm.at[0, 1, :, rows], x_v.at[1, :, rows]),
            ]
        )
    load_sel = load(sel_hbm, sel_v)
    load_back = load(tab_hbm.at[pl.ds(GROUP, GROUP)], back_v)

    barrier = pltpu.get_barrier_semaphore()
    for d in range(1, SIDE):
        pl.semaphore_signal(barrier, inc=1, device_id=at((y + d) % SIDE, z), device_id_type=MESH)
        pl.semaphore_signal(barrier, inc=1, device_id=at(y, (z + d) % SIDE), device_id_type=MESH)

    def first(axis, d, c):
        part = pl.ds(c * PER_CHUNK, PER_CHUNK)
        to = ((z if axis == 0 else y) + d) % SIDE
        return pltpu.make_async_remote_copy(
            src_ref=(zsend if axis == 0 else ysend).at[to, part],
            dst_ref=(zin if axis == 0 else yin).at[z if axis == 0 else y, part],
            send_sem=r1s.at[axis], recv_sem=r1r.at[axis, c],
            device_id=at(y, to) if axis == 0 else at(to, z), device_id_type=MESH,
        )

    tn = (((0,), (0,)), ((), ()))
    lane = lax.broadcasted_iota(jnp.int32, (CAP, SPAN), 1)
    ones = jnp.ones((SIDE * CAP, COLS), BF16)
    owner_lane = lax.broadcasted_iota(jnp.int32, (CAP, SIDE * SIDE), 1)
    load_own.wait()
    for s in range(STEPS):
        own = own_v[s]
        own = jnp.where(own >= 0, own + (owner_lane % SIDE) * PER_OWNER, -1)
        for g in range(SIDE):
            picks = [
                (own[:, g * SIDE + q : g * SIDE + q + 1] == lane).astype(F32)
                for q in range(SIDE)
            ]
            onehot = jnp.concatenate(picks, axis=0).astype(BF16)
            pick_v[s, g] = onehot
            keep_v[s, g] = 1.0 - dot(onehot, ones, tn)
    load_g.wait()
    load_tab.wait()
    for half in range(HALVES):
        groups = range(half * SIDE // HALVES, (half + 1) * SIDE // HALVES)
        load_half[half][0].wait()
        load_half[half][1].wait()
        for g in groups:
            rows = pl.ds(g * SPAN, SPAN)
            f_v[0, g] = DECAY * m_v[rows, :] + dot(x_v[0, :, rows], g_v[0], tn)
        load_half[half][2].wait()
        for g in groups:
            rows = pl.ds(g * SPAN, SPAN)
            f_v[1, g] = dot(x_v[1, :, rows], g_v[1], tn)
        for s in range(STEPS):
            for g in groups:
                c = blocks_apply(tab_v[...], f_v[s, g])
                if s:
                    c = c + DECAY * kept_v[g]
                packed = folded(dot(pick_v[s, g], split(c)))
                kept_v[g] = keep_v[s, g] * c
                for q in range(SIDE):
                    tile = packed[q * CAP : (q + 1) * CAP]
                    if (g + q) % 2 == 0:
                        zsend[q, g // 2, s * CAP : (s + 1) * CAP, :] = tile
                    else:
                        ysend[g, q // 2, s * CAP : (s + 1) * CAP, :] = tile
        if half == 0:
            pl.semaphore_wait(barrier, 2 * (SIDE - 1))
        for c in range(CHUNKS):
            if c * HALVES // CHUNKS == half:
                for d in FAR_FIRST:
                    first(0, d, c).start()
        if HALVES == 1:
            for c in range(CHUNKS):
                for d in FAR_FIRST:
                    first(1, d, c).start()
        else:
            for c in range(CHUNKS):
                for g in groups:

                    @pl.when(y != g)
                    def _():
                        first(1, (g - y + SIDE) % SIDE, c).start()

    zin[z] = zsend[z]
    yin[y] = ysend[y]

    load_sel.wait()
    load_back.wait()
    pick_row = lax.broadcasted_iota(jnp.int32, (COLS, SIDE * SIDE), 0)
    pick_lane = lax.broadcasted_iota(jnp.int32, (COLS, SIDE * SIDE), 1)
    place = (lax.broadcasted_iota(jnp.int32, (COLS, COLS), 0) % PER_OWNER).astype(F32)
    nt = (((1,), (1,)), ((), ()))

    def scatter_table(listed, owner):
        chooser = (pick_lane == owner).astype(F32).astype(BF16)
        wanted = dot(chooser, listed.astype(F32).astype(BF16), nt)
        return (wanted == place).astype(F32).astype(BF16)

    along_z = sel_v[pl.ds(y * SIDE, SIDE)].reshape(COLS, SIDE * SIDE)
    along_y = jnp.concatenate(
        [sel_v[q * SIDE + z].reshape(STEPS * CAP, SIDE * SIDE) for q in range(SIDE)], axis=0
    )
    index = pick_row // PER_OWNER
    table_z = scatter_table(along_z, (2 * index + z % 2) * SIDE + z)
    table_y = scatter_table(along_y, y * SIDE + 2 * index + (y + 1) % 2)

    backward = back_v[...]
    for g in range(SIDE):
        mom_ref[g * SPAN : (g + 1) * SPAN, :] = blocks_apply(backward, kept_v[g])

    def second(axis, i):
        to = 2 * i + (z % 2 if axis == 0 else (y + 1) % 2)
        return to, pltpu.make_async_remote_copy(
            src_ref=(pz if axis == 0 else py).at[i],
            dst_ref=p2in.at[y if axis == 0 else z],
            send_sem=p2s, recv_sem=p2r,
            device_id=at(to, z) if axis == 0 else at(y, to), device_id_type=MESH,
        )

    def others(ref, send_sem, recv_sem):
        return pltpu.make_async_remote_copy(
            src_ref=ref, dst_ref=ref, send_sem=send_sem, recv_sem=recv_sem,
            device_id=at((y + 1) % SIDE, z), device_id_type=MESH,
        )

    def await_recv(ref, sem):
        others(ref, p2s, sem).wait_recv()

    def await_send(ref, sem):
        others(ref, sem, p2r).wait_send()

    for c in range(CHUNKS):
        part = pl.ds(c * PER_CHUNK, PER_CHUNK)
        for axis in range(2):
            await_recv((zin if axis == 0 else yin).at[pl.ds(0, SIDE - 1), part], r1r.at[axis, c])
        for i in range(c * PER_CHUNK, (c + 1) * PER_CHUNK):
            block = slice(i * PER_OWNER, (i + 1) * PER_OWNER)
            for axis in range(2):
                arrived = (zin if axis == 0 else yin)[:, i].reshape(COLS, COLS)
                table = table_z if axis == 0 else table_y
                (pz if axis == 0 else py)[i] = folded(dot(table[block], split(arrived)))
        for i in range(c * PER_CHUNK, (c + 1) * PER_CHUNK):
            for axis in range(2):
                to, copy = second(axis, i)
                here = y if axis == 0 else z

                @pl.when(to != here)
                def _():
                    copy.start()

                @pl.when(to == here)
                def _():
                    p2in[here] = (pz if axis == 0 else py)[i]

    def done1():
        await_send(zsend.at[pl.ds(0, SIDE - 1)], r1s.at[0])
        await_send(ysend.at[pl.ds(0, SIDE - 1)], r1s.at[1])

    along = y + par * (z - y)
    line = z + par * (y - z)
    mine = along // 2
    await_recv(p2in.at[pl.ds(0, SIDE - 1)], p2r)
    total = p2in[0]
    for k in range(1, SIDE):
        total = total + p2in[k]
    tout[...] = total
    u_v[par, line, mine] = total

    def done2():
        done1()
        await_send(p2in.at[pl.ds(0, SIDE - 1)], p2s)

    def third(d):
        to_y = (y + (1 - par) * d) % SIDE
        to_z = (z + par * d) % SIDE
        return pltpu.make_async_remote_copy(
            src_ref=tout, dst_ref=u_v.at[par, line, mine],
            send_sem=a1s, recv_sem=a1r.at[par, mine],
            device_id=at(to_y, to_z), device_id_type=MESH,
        )

    for d in FAR_FIRST:
        third(d).start()

    def third_arrived(axis, i):
        where = z if axis == 0 else y

        @pl.when(jnp.logical_or(par != axis, mine != i))
        def _():
            await_recv(u_v.at[axis, where, i], a1r.at[axis, i])

    def spread(axis, way, hop, behind, first_block, blocks):
        pos = z if axis == 0 else y
        step = 1 if way == 0 else SIDE - 1
        source = (pos + behind * (SIDE - step)) % SIDE
        to = (pos + hop * step) % SIDE
        block = u_v.at[axis, source, pl.ds(first_block, blocks)]
        slot = 2 * (behind + hop - 1) + way
        return pltpu.make_async_remote_copy(
            src_ref=block, dst_ref=block,
            send_sem=a2s.at[axis], recv_sem=a2r.at[axis, slot, first_block // 2],
            device_id=at(y, to) if axis == 0 else at(to, z), device_id_type=MESH,
        )

    def spread_arrived(axis, way, distance, first_block, blocks):
        pos = z if axis == 0 else y
        step = 1 if way == 0 else SIDE - 1
        source = (pos + distance * (SIDE - step)) % SIDE
        block = u_v.at[axis, source, pl.ds(first_block, blocks)]
        await_recv(block, a2r.at[axis, 2 * (distance - 1) + way, first_block // 2])

    for half in range(2):
        for axis in range(2):
            for i in (2 * half, 2 * half + 1):
                third_arrived(axis, i)
            for way in range(2):
                spread(axis, way, 2, 0, 2 * half, 2).start()
    for axis in range(2):
        for way in range(2):
            spread(axis, way, 1, 0, 0, 4).start()
    for half in range(2):
        for axis in range(2):
            for way in range(2):
                spread_arrived(axis, way, 2, 2 * half, 2)
                if half == way:
                    spread(axis, way, 2, 2, 2 * half, 2).start()
                spread(axis, way, 1, 2, 2 * half, 2).start()
    done2()
    await_send(p2in.at[pl.ds(0, SIDE - 1)], a1s)
    for axis in range(2):
        for way in range(2):
            spread_arrived(axis, way, 1, 0, 4)
    for half in range(2):
        for axis in range(2):
            for way in range(2):
                spread_arrived(axis, way, 3, 2 * half, 2)
                if half == way:
                    spread_arrived(axis, way, 4, 2 * half, 2)
    for axis in range(2):
        await_send(u_v.at[axis, pl.ds(0, SIDE - 1)], a2s.at[axis])


def deliver(u_ref, mom_ref, back_ref, upd_out, mom_out, upd_v, sem):
    momentum = pltpu.make_async_copy(mom_ref, mom_out, sem.at[SIDE])
    momentum.start()
    copies = []
    for g in range(SIDE):
        rows = pl.ds(g * SPAN, SPAN)
        parts = [
            u_ref[0, q, g // 2] if (g + q) % 2 == 0 else u_ref[1, g, q // 2]
            for q in range(SIDE)
        ]
        block = blocks_apply(back_ref[...], jnp.concatenate(parts, axis=0))
        upd_v[rows, :] = block.astype(BF16)
        copies.append(pltpu.make_async_copy(upd_v.at[rows], upd_out.at[rows], sem.at[g]))
        copies[-1].start()
    for copy in copies:
        copy.wait()
    momentum.wait()


def per_device(inputs, grad_out, momentum, select):
    table = jnp.asarray(transform_tables())
    listed = jnp.transpose(select, (0, 1, 3, 2))
    hbm = pl.BlockSpec(memory_space=pl.ANY)
    vmem = pl.BlockSpec(memory_space=pltpu.VMEM)
    operands = [
        pltpu.with_memory_space_constraint(v, pltpu.HBM)
        for v in (inputs, grad_out, momentum, listed, table)
    ]
    outs = (
        jax.ShapeDtypeStruct((ROWS, COLS), BF16),
        jax.ShapeDtypeStruct((ROWS, COLS), F32),
    )
    gathered, new_momentum, back = pl.pallas_call(
        kernel,
        out_shape=(
            jax.ShapeDtypeStruct((2, SIDE, 4, PER_OWNER, COLS), F32),
            outs[1],
            jax.ShapeDtypeStruct((GROUP, SPAN), BF16),
        ),
        in_specs=[hbm] * 5,
        out_specs=(vmem, vmem, vmem),
        scratch_shapes=[
            pltpu.VMEM((STEPS, TOK, ROWS), BF16),
            pltpu.VMEM((STEPS, TOK, COLS), BF16),
            pltpu.VMEM((ROWS, COLS), F32),
            pltpu.VMEM((SIDE * SIDE, STEPS, CAP, SIDE * SIDE), jnp.int32),
            pltpu.VMEM((STEPS, CAP, SIDE * SIDE), jnp.int32),
            pltpu.VMEM((GROUP, SPAN), BF16),
            pltpu.VMEM((STEPS, SIDE, SPAN, COLS), F32),
            pltpu.VMEM((SIDE, SPAN, COLS), F32),
            pltpu.VMEM((STEPS, SIDE, SIDE * CAP, SPAN), BF16),
            pltpu.VMEM((STEPS, SIDE, SPAN, COLS), F32),
            pltpu.VMEM((SIDE, 4, STEPS * CAP, COLS), F32),
            pltpu.VMEM((SIDE, 4, STEPS * CAP, COLS), F32),
            pltpu.VMEM((SIDE, 4, STEPS * CAP, COLS), F32),
            pltpu.VMEM((SIDE, 4, STEPS * CAP, COLS), F32),
            pltpu.VMEM((4, PER_OWNER, COLS), F32),
            pltpu.VMEM((4, PER_OWNER, COLS), F32),
            pltpu.VMEM((SIDE, PER_OWNER, COLS), F32),
            pltpu.VMEM((PER_OWNER, COLS), F32),
            pltpu.SemaphoreType.DMA((5 + 3 * HALVES,)),
            pltpu.SemaphoreType.DMA((2,)),
            pltpu.SemaphoreType.DMA((2, CHUNKS)),
            pltpu.SemaphoreType.DMA,
            pltpu.SemaphoreType.DMA,
            pltpu.SemaphoreType.DMA,
            pltpu.SemaphoreType.DMA((2, 4)),
            pltpu.SemaphoreType.DMA((2,)),
            pltpu.SemaphoreType.DMA((2, 8, 2)),
        ],
        compiler_params=pltpu.CompilerParams(
            collective_id=0, has_side_effects=True, vmem_limit_bytes=40 << 20
        ),
    )(*operands)
    update, new_momentum = pl.pallas_call(
        deliver,
        out_shape=outs,
        in_specs=[vmem] * 3,
        out_specs=(hbm, hbm),
        scratch_shapes=[
            pltpu.VMEM((ROWS, COLS), BF16),
            pltpu.SemaphoreType.DMA((SIDE + 1,)),
        ],
        compiler_params=pltpu.CompilerParams(vmem_limit_bytes=16 << 20),
    )(gathered, new_momentum, back)
    return (update, new_momentum[None])


def solution(mesh):
    return jax.shard_map(
        per_device,
        mesh=mesh,
        in_specs=(
            P("dp", None, None, None),
            P("dp", None, None, "mp"),
            P("dp", None, "mp"),
            P(None, None, None, "mp"),
        ),
        out_specs=(P(None, "mp"), P("dp", None, "mp")),
        check_vma=False,
    )
```

```python
import jax
import jax.numpy as jnp
import numpy as np
from jax import lax
from jax.experimental import pallas as pl
from jax.experimental.pallas import tpu as pltpu
from jax.sharding import PartitionSpec as P

GROUP = 64
DECAY = 0.999
SIDE = 8
PER_OWNER = 32
CAP = 8
STEPS = 2
ROWS = 2048
COLS = 128
TOK = 256
SPAN = 256
BF16 = jnp.bfloat16
F32 = jnp.float32
MESH = pl.DeviceIdType.MESH
FAR_FIRST = (4, 3, 5, 2, 6, 1, 7)
NEAR_EVEN = (0, 2, -2, 4)
NEAR_ODD = (1, -1, 3, -3)


def transform_tables():
    u = np.arange(GROUP)[:, None].astype(np.float64)
    i = np.arange(GROUP)[None, :].astype(np.float64)
    scale = np.where(u == 0, np.sqrt(1.0 / GROUP), np.sqrt(2.0 / GROUP))
    dct = (scale * np.cos(np.pi * (2 * i + 1) * u / (2 * GROUP))).astype(np.float32)

    def parts(table):
        high = table.astype(BF16)
        low = (table - high.astype(np.float32)).astype(BF16)
        return np.concatenate([high, high, low, np.zeros_like(low)], 1)

    return np.concatenate([parts(dct), parts(dct.T)], 0)


def split(x):
    high = x.astype(BF16)
    low = (x - high.astype(F32)).astype(BF16)
    return jnp.concatenate([high, low], axis=1)


def dot(a, b, dims=(((1,), (0,)), ((), ()))):
    return lax.dot_general(a, b, dims, preferred_element_type=F32)


def folded(x):
    return x[:, :COLS] + x[:, COLS:]


def pair_products(tables, x):
    high = x.astype(BF16)
    low = (x - high.astype(F32)).astype(BF16)

    def stacked(b):
        rows = slice(b * GROUP, (b + 1) * GROUP)
        return jnp.concatenate([high[rows], low[rows], high[rows]], axis=0)

    return [
        dot(tables[p], jnp.concatenate([stacked(2 * p), stacked(2 * p + 1)], axis=1))
        for p in range(SPAN // GROUP // 2)
    ]


def blocks_of(products):
    out = []
    for r in products:
        out += [r[:GROUP, :COLS], r[:GROUP, COLS:]]
    return jnp.concatenate(out, axis=0)


def blocks_apply(table, x):
    return blocks_of(pair_products([table[:, :DEPTH]] * 2, x))


DEPTH = 3 * GROUP
CHUNKS = 4
HALVES = 2
PER_CHUNK = 4 // CHUNKS


def kernel(
    x_hbm, g_hbm, m_hbm, sel_hbm, tab_hbm,
    u_v, mom_ref, back_v,
    x_v, g_v, m_v, sel_v, own_v, tab_v, f_v, kept_v, pick_v, tsel_v, ext_v,
    zsend, ysend, zin, yin, pz, py, p2in, tout,
    load_sem, r1s, r1r, p2s, p2r, a1s, a1r, a2s, a2r,
):
    me = lax.axis_index("dp")
    mp = lax.axis_index("mp")
    y = me // SIDE
    z = me % SIDE
    par = (y + z) % 2

    def at(yy, zz):
        return (yy * SIDE + zz, mp)

    barrier = pltpu.get_barrier_semaphore()
    for d in range(1, SIDE):
        pl.semaphore_signal(barrier, inc=1, device_id=at((y + d) % SIDE, z), device_id_type=MESH)
        pl.semaphore_signal(barrier, inc=1, device_id=at(y, (z + d) % SIDE), device_id_type=MESH)

    loads = []

    def load(src, dst):
        copy = pltpu.make_async_copy(src, dst, load_sem.at[len(loads)])
        copy.start()
        loads.append(copy)
        return copy

    half_rows = ROWS // HALVES
    load_own = load(sel_hbm.at[me], own_v)
    load_g = load(g_hbm.at[0], g_v)
    load_tab = load(tab_hbm.at[pl.ds(0, GROUP)], tab_v)
    load_half = []
    for half in range(HALVES):
        rows = pl.ds(half * half_rows, half_rows)
        load_half.append(
            [
                load(x_hbm.at[0, 0, :, rows], x_v.at[0, :, rows]),
                load(m_hbm.at[0, rows], m_v.at[rows]),
                load(x_hbm.at[0, 1, :, rows], x_v.at[1, :, rows]),
            ]
        )
    load_sel = load(sel_hbm, sel_v)
    load_back = load(tab_hbm.at[pl.ds(GROUP, GROUP)], back_v)

    def first(axis, d, c):
        part = pl.ds(c * PER_CHUNK, PER_CHUNK)
        to = ((z if axis == 0 else y) + d) % SIDE
        return pltpu.make_async_remote_copy(
            src_ref=(zsend if axis == 0 else ysend).at[to, part],
            dst_ref=(zin if axis == 0 else yin).at[z if axis == 0 else y, part],
            send_sem=r1s.at[axis], recv_sem=r1r.at[axis, c],
            device_id=at(y, to) if axis == 0 else at(to, z), device_id_type=MESH,
        )

    def send_half(half):
        for c in range(CHUNKS):
            if c * HALVES // CHUNKS == half:
                for d in FAR_FIRST:
                    first(0, d, c).start()
        for c in range(CHUNKS):
            for g in range(half * SIDE // HALVES, (half + 1) * SIDE // HALVES):

                @pl.when(y != g)
                def _():
                    first(1, (g - y + SIDE) % SIDE, c).start()

    tn = (((0,), (0,)), ((), ()))
    lane = lax.broadcasted_iota(jnp.int32, (CAP, SPAN), 1)
    ones = jnp.ones((SIDE * CAP, COLS), BF16)
    owner_lane = lax.broadcasted_iota(jnp.int32, (CAP, SIDE * SIDE), 1)
    load_own.wait()
    load_tab.wait()
    table = tab_v[...]
    stack = jnp.concatenate([table] * (SPAN // GROUP), axis=0)
    second_list = own_v[1]
    again = second_list == own_v[0, 0:1, :]
    for j in range(1, CAP):
        again = jnp.logical_or(again, second_list == own_v[0, j : j + 1, :])
    fresh = jnp.where(again, 0.0, DECAY).astype(F32)
    for s in range(STEPS):
        own = own_v[s]
        own = jnp.where(own >= 0, own + (owner_lane % SIDE) * PER_OWNER, -1)
        for g in range(SIDE):
            picks = [
                (own[:, g * SIDE + q : g * SIDE + q + 1] == lane).astype(F32)
                for q in range(SIDE)
            ]
            onehot = jnp.concatenate(picks, axis=0).astype(BF16)
            pick_v[s, g] = onehot
            tsel_v[s, g] = dot(onehot, stack).astype(BF16)
    load_g.wait()

    def rows_of(s, g, p):
        return tsel_v[s, g, p * 4 * CAP : (p + 1) * 4 * CAP, :DEPTH]

    def tile_of(products, base, q):
        side = (q // 2) % 2 * COLS
        top = base + q % 4 * CAP
        return products[q // 4][top : top + CAP, side : side + COLS]

    for half in range(HALVES):
        groups = range(half * SIDE // HALVES, (half + 1) * SIDE // HALVES)
        load_half[half][0].wait()
        load_half[half][1].wait()
        for g in groups:
            rows = pl.ds(g * SPAN, SPAN)
            f_v[0, g] = DECAY * m_v[rows, :] + dot(x_v[0, :, rows], g_v[0], tn)
        load_half[half][2].wait()
        for g in groups:
            rows = pl.ds(g * SPAN, SPAN)
            f_v[1, g] = dot(x_v[1, :, rows], g_v[1], tn)
        for s in range(STEPS):
            for g in groups:
                tables = [
                    jnp.concatenate(
                        [table[:, :DEPTH]] + [rows_of(t, g, p) for t in range(s, STEPS)],
                        axis=0,
                    )
                    for p in range(2)
                ]
                products = pair_products(tables, f_v[s, g])
                f_v[s, g] = blocks_of(products)
                for q in range(SIDE):
                    tile = tile_of(products, GROUP, q)
                    if s == 0:
                        o = g * SIDE + q
                        ext_v[g, q] = fresh[:, o : o + 1] * tile_of(
                            products, GROUP + 4 * CAP, q
                        )
                    else:
                        tile = tile + ext_v[g, q]
                    if (g + q) % 2 == 0:
                        zsend[q, g // 2, s * CAP : (s + 1) * CAP, :] = tile
                    else:
                        ysend[g, q // 2, s * CAP : (s + 1) * CAP, :] = tile
        if half == 0:
            pl.semaphore_wait(barrier, 2 * (SIDE - 1))
        send_half(half)

    zin[z] = zsend[z]
    yin[y] = ysend[y]

    load_sel.wait()
    load_back.wait()
    pick_row = lax.broadcasted_iota(jnp.int32, (COLS, SIDE * SIDE), 0)
    pick_lane = lax.broadcasted_iota(jnp.int32, (COLS, SIDE * SIDE), 1)
    place = (lax.broadcasted_iota(jnp.int32, (COLS, COLS), 0) % PER_OWNER).astype(F32)
    nt = (((1,), (1,)), ((), ()))

    def scatter_table(listed, owner):
        chooser = (pick_lane == owner).astype(F32).astype(BF16)
        wanted = dot(chooser, listed.astype(F32).astype(BF16), nt)
        return (wanted == place).astype(F32).astype(BF16)

    along_z = sel_v[pl.ds(y * SIDE, SIDE)].reshape(COLS, SIDE * SIDE)
    along_y = jnp.concatenate(
        [sel_v[q * SIDE + z].reshape(STEPS * CAP, SIDE * SIDE) for q in range(SIDE)], axis=0
    )
    index = pick_row // PER_OWNER
    table_z = scatter_table(along_z, (2 * index + z % 2) * SIDE + z)
    table_y = scatter_table(along_y, y * SIDE + 2 * index + (y + 1) % 2)

    backward = back_v[...]
    for g in range(SIDE):
        keep = [1.0 - dot(pick_v[s, g], ones, tn) for s in range(STEPS)]
        kept_v[g] = keep[1] * (DECAY * keep[0] * f_v[0, g] + f_v[1, g])
    for g in range(SIDE):
        mom_ref[g * SPAN : (g + 1) * SPAN, :] = blocks_apply(backward, kept_v[g])

    def second(axis, i):
        to = 2 * i + (z % 2 if axis == 0 else (y + 1) % 2)
        return to, pltpu.make_async_remote_copy(
            src_ref=(pz if axis == 0 else py).at[i],
            dst_ref=p2in.at[y if axis == 0 else z],
            send_sem=p2s, recv_sem=p2r,
            device_id=at(to, z) if axis == 0 else at(y, to), device_id_type=MESH,
        )

    def others(ref, send_sem, recv_sem):
        return pltpu.make_async_remote_copy(
            src_ref=ref, dst_ref=ref, send_sem=send_sem, recv_sem=recv_sem,
            device_id=at((y + 1) % SIDE, z), device_id_type=MESH,
        )

    def await_recv(ref, sem):
        others(ref, p2s, sem).wait_recv()

    def await_send(ref, sem):
        others(ref, sem, p2r).wait_send()

    for c in range(CHUNKS):
        part = pl.ds(c * PER_CHUNK, PER_CHUNK)
        for axis in range(2):
            await_recv((zin if axis == 0 else yin).at[pl.ds(0, SIDE - 1), part], r1r.at[axis, c])
        for i in range(c * PER_CHUNK, (c + 1) * PER_CHUNK):
            block = slice(i * PER_OWNER, (i + 1) * PER_OWNER)
            for axis in range(2):
                arrived = (zin if axis == 0 else yin)[:, i].reshape(COLS, COLS)
                table = table_z if axis == 0 else table_y
                (pz if axis == 0 else py)[i] = folded(dot(table[block], split(arrived)))
        for i in range(c * PER_CHUNK, (c + 1) * PER_CHUNK):
            for axis in range(2):
                to, copy = second(axis, i)
                here = y if axis == 0 else z

                @pl.when(to != here)
                def _():
                    copy.start()

                @pl.when(to == here)
                def _():
                    p2in[here] = (pz if axis == 0 else py)[i]

    def done1():
        await_send(zsend.at[pl.ds(0, SIDE - 1)], r1s.at[0])
        await_send(ysend.at[pl.ds(0, SIDE - 1)], r1s.at[1])

    along = y + par * (z - y)
    line = z + par * (y - z)
    mine = along // 2
    await_recv(p2in.at[pl.ds(0, SIDE - 1)], p2r)
    total = p2in[0]
    for k in range(1, SIDE):
        total = total + p2in[k]
    tout[...] = total
    u_v[par, line, mine] = total

    def done2():
        done1()
        await_send(p2in.at[pl.ds(0, SIDE - 1)], p2s)

    def third(d):
        to_y = (y + (1 - par) * d) % SIDE
        to_z = (z + par * d) % SIDE
        return pltpu.make_async_remote_copy(
            src_ref=tout, dst_ref=u_v.at[par, line, mine],
            send_sem=a1s, recv_sem=a1r.at[par, mine],
            device_id=at(to_y, to_z), device_id_type=MESH,
        )

    for d in FAR_FIRST:
        third(d).start()

    def third_arrived(axis, i):
        where = z if axis == 0 else y

        @pl.when(jnp.logical_or(par != axis, mine != i))
        def _():
            await_recv(u_v.at[axis, where, i], a1r.at[axis, i])

    def spread(axis, way, hop, behind, first_block, blocks):
        pos = z if axis == 0 else y
        step = 1 if way == 0 else SIDE - 1
        source = (pos + behind * (SIDE - step)) % SIDE
        to = (pos + hop * step) % SIDE
        block = u_v.at[axis, source, pl.ds(first_block, blocks)]
        slot = 2 * (behind + hop - 1) + way
        return pltpu.make_async_remote_copy(
            src_ref=block, dst_ref=block,
            send_sem=a2s.at[axis], recv_sem=a2r.at[axis, slot, first_block // 2],
            device_id=at(y, to) if axis == 0 else at(to, z), device_id_type=MESH,
        )

    def spread_arrived(axis, way, distance, first_block, blocks):
        pos = z if axis == 0 else y
        step = 1 if way == 0 else SIDE - 1
        source = (pos + distance * (SIDE - step)) % SIDE
        block = u_v.at[axis, source, pl.ds(first_block, blocks)]
        await_recv(block, a2r.at[axis, 2 * (distance - 1) + way, first_block // 2])

    for half in range(2):
        for axis in range(2):
            for i in (2 * half, 2 * half + 1):
                third_arrived(axis, i)
            for way in range(2):
                spread(axis, way, 2, 0, 2 * half, 2).start()
    for axis in range(2):
        for way in range(2):
            spread(axis, way, 1, 0, 0, 4).start()
    for half in range(2):
        for axis in range(2):
            for way in range(2):
                spread_arrived(axis, way, 2, 2 * half, 2)
                if half == way:
                    spread(axis, way, 2, 2, 2 * half, 2).start()
                spread(axis, way, 1, 2, 2 * half, 2).start()
    done2()
    await_send(p2in.at[pl.ds(0, SIDE - 1)], a1s)
    for axis in range(2):
        for way in range(2):
            spread_arrived(axis, way, 1, 0, 4)
    for half in range(2):
        for axis in range(2):
            for way in range(2):
                spread_arrived(axis, way, 3, 2 * half, 2)
                if half == way:
                    spread_arrived(axis, way, 4, 2 * half, 2)
    for axis in range(2):
        await_send(u_v.at[axis, pl.ds(0, SIDE - 1)], a2s.at[axis])


def deliver(u_ref, mom_ref, back_ref, upd_out, mom_out, upd_v, sem):
    momentum = pltpu.make_async_copy(mom_ref, mom_out, sem.at[SIDE])
    momentum.start()
    copies = []
    for g in range(SIDE):
        rows = pl.ds(g * SPAN, SPAN)
        parts = [
            u_ref[0, q, g // 2] if (g + q) % 2 == 0 else u_ref[1, g, q // 2]
            for q in range(SIDE)
        ]
        block = blocks_apply(back_ref[...], jnp.concatenate(parts, axis=0))
        upd_v[rows, :] = block.astype(BF16)
        copies.append(pltpu.make_async_copy(upd_v.at[rows], upd_out.at[rows], sem.at[g]))
        copies[-1].start()
    for copy in copies:
        copy.wait()
    momentum.wait()


def per_device(inputs, grad_out, momentum, select):
    table = jnp.asarray(transform_tables())
    listed = jnp.transpose(select, (0, 1, 3, 2))
    hbm = pl.BlockSpec(memory_space=pl.ANY)
    vmem = pl.BlockSpec(memory_space=pltpu.VMEM)
    operands = [
        pltpu.with_memory_space_constraint(v, pltpu.HBM)
        for v in (inputs, grad_out, momentum, listed, table)
    ]
    outs = (
        jax.ShapeDtypeStruct((ROWS, COLS), BF16),
        jax.ShapeDtypeStruct((ROWS, COLS), F32),
    )
    gathered, new_momentum, back = pl.pallas_call(
        kernel,
        out_shape=(
            jax.ShapeDtypeStruct((2, SIDE, 4, PER_OWNER, COLS), F32),
            outs[1],
            jax.ShapeDtypeStruct((GROUP, SPAN), BF16),
        ),
        in_specs=[hbm] * 5,
        out_specs=(vmem, vmem, vmem),
        scratch_shapes=[
            pltpu.VMEM((STEPS, TOK, ROWS), BF16),
            pltpu.VMEM((STEPS, TOK, COLS), BF16),
            pltpu.VMEM((ROWS, COLS), F32),
            pltpu.VMEM((SIDE * SIDE, STEPS, CAP, SIDE * SIDE), jnp.int32),
            pltpu.VMEM((STEPS, CAP, SIDE * SIDE), jnp.int32),
            pltpu.VMEM((GROUP, SPAN), BF16),
            pltpu.VMEM((STEPS, SIDE, SPAN, COLS), F32),
            pltpu.VMEM((SIDE, SPAN, COLS), F32),
            pltpu.VMEM((STEPS, SIDE, SIDE * CAP, SPAN), BF16),
            pltpu.VMEM((STEPS, SIDE, SIDE * CAP, SPAN), BF16),
            pltpu.VMEM((SIDE, SIDE, CAP, COLS), F32),
            pltpu.VMEM((SIDE, 4, STEPS * CAP, COLS), F32),
            pltpu.VMEM((SIDE, 4, STEPS * CAP, COLS), F32),
            pltpu.VMEM((SIDE, 4, STEPS * CAP, COLS), F32),
            pltpu.VMEM((SIDE, 4, STEPS * CAP, COLS), F32),
            pltpu.VMEM((4, PER_OWNER, COLS), F32),
            pltpu.VMEM((4, PER_OWNER, COLS), F32),
            pltpu.VMEM((SIDE, PER_OWNER, COLS), F32),
            pltpu.VMEM((PER_OWNER, COLS), F32),
            pltpu.SemaphoreType.DMA((5 + 3 * HALVES,)),
            pltpu.SemaphoreType.DMA((2,)),
            pltpu.SemaphoreType.DMA((2, CHUNKS)),
            pltpu.SemaphoreType.DMA,
            pltpu.SemaphoreType.DMA,
            pltpu.SemaphoreType.DMA,
            pltpu.SemaphoreType.DMA((2, 4)),
            pltpu.SemaphoreType.DMA((2,)),
            pltpu.SemaphoreType.DMA((2, 8, 2)),
        ],
        compiler_params=pltpu.CompilerParams(
            collective_id=0, has_side_effects=True, vmem_limit_bytes=40 << 20
        ),
    )(*operands)
    update, new_momentum = pl.pallas_call(
        deliver,
        out_shape=outs,
        in_specs=[vmem] * 3,
        out_specs=(hbm, hbm),
        scratch_shapes=[
            pltpu.VMEM((ROWS, COLS), BF16),
            pltpu.SemaphoreType.DMA((SIDE + 1,)),
        ],
        compiler_params=pltpu.CompilerParams(vmem_limit_bytes=16 << 20),
    )(gathered, new_momentum, back)
    return (update, new_momentum[None])


def solution(mesh):
    return jax.shard_map(
        per_device,
        mesh=mesh,
        in_specs=(
            P("dp", None, None, None),
            P("dp", None, None, "mp"),
            P("dp", None, "mp"),
            P(None, None, None, "mp"),
        ),
        out_specs=(P(None, "mp"), P("dp", None, "mp")),
        check_vma=False,
    )
```

```python
import jax
import jax.numpy as jnp
import numpy as np
from jax import lax
from jax.experimental import pallas as pl
from jax.experimental.pallas import tpu as pltpu
from jax.sharding import PartitionSpec as P

GROUP = 64
DECAY = 0.999
SIDE = 8
PER_OWNER = 32
CAP = 8
STEPS = 2
ROWS = 2048
COLS = 128
TOK = 256
SPAN = 256
BF16 = jnp.bfloat16
F32 = jnp.float32
MESH = pl.DeviceIdType.MESH
FAR_FIRST = (4, 3, 5, 2, 6, 1, 7)
NEAR_EVEN = (0, 2, -2, 4)
NEAR_ODD = (1, -1, 3, -3)


def transform_tables():
    u = np.arange(GROUP)[:, None].astype(np.float64)
    i = np.arange(GROUP)[None, :].astype(np.float64)
    scale = np.where(u == 0, np.sqrt(1.0 / GROUP), np.sqrt(2.0 / GROUP))
    dct = (scale * np.cos(np.pi * (2 * i + 1) * u / (2 * GROUP))).astype(np.float32)

    def parts(table):
        high = table.astype(BF16)
        low = (table - high.astype(np.float32)).astype(BF16)
        return np.concatenate([high, high, low, np.zeros_like(low)], 1)

    return np.concatenate([parts(dct), parts(dct.T)], 0)


def split(x):
    high = x.astype(BF16)
    low = (x - high.astype(F32)).astype(BF16)
    return jnp.concatenate([high, low], axis=1)


def dot(a, b, dims=(((1,), (0,)), ((), ()))):
    return lax.dot_general(a, b, dims, preferred_element_type=F32)


def folded(x):
    return x[:, :COLS] + x[:, COLS:]


def pair_products(tables, x):
    high = x.astype(BF16)
    low = (x - high.astype(F32)).astype(BF16)

    def stacked(b):
        rows = slice(b * GROUP, (b + 1) * GROUP)
        return jnp.concatenate([high[rows], low[rows], high[rows]], axis=0)

    return [
        dot(tables[p], jnp.concatenate([stacked(2 * p), stacked(2 * p + 1)], axis=1))
        for p in range(SPAN // GROUP // 2)
    ]


def blocks_of(products):
    out = []
    for r in products:
        out += [r[:GROUP, :COLS], r[:GROUP, COLS:]]
    return jnp.concatenate(out, axis=0)


def blocks_apply(table, x):
    return blocks_of(pair_products([table[:, :DEPTH]] * 2, x))


DEPTH = 3 * GROUP
CHUNKS = 4
HALVES = 2
PER_CHUNK = 4 // CHUNKS


def kernel(
    x_hbm, g_hbm, m_hbm, sel_hbm, tab_hbm,
    u_v, mom_ref, back_v,
    x_v, g_v, m_v, sel_v, own_v, tab_v, f_v, kept_v, pick_v, tsel_v, ext_v,
    zsend, ysend, zin, yin, pz, py, p2in, tout,
    load_sem, r1s, r1r, p2s, p2r, a1s, a1r, a2s, a2r,
):
    me = lax.axis_index("dp")
    mp = lax.axis_index("mp")
    y = me // SIDE
    z = me % SIDE
    par = (y + z) % 2

    def at(yy, zz):
        return (yy * SIDE + zz, mp)

    barrier = pltpu.get_barrier_semaphore()
    for d in range(1, SIDE):
        pl.semaphore_signal(barrier, inc=1, device_id=at((y + d) % SIDE, z), device_id_type=MESH)
        pl.semaphore_signal(barrier, inc=1, device_id=at(y, (z + d) % SIDE), device_id_type=MESH)

    loads = []

    def load(src, dst):
        copy = pltpu.make_async_copy(src, dst, load_sem.at[len(loads)])
        copy.start()
        loads.append(copy)
        return copy

    half_rows = ROWS // HALVES
    load_own = load(sel_hbm.at[me], own_v)
    load_g = load(g_hbm.at[0], g_v)
    load_tab = load(tab_hbm.at[pl.ds(0, GROUP)], tab_v)
    load_half = []
    for half in range(HALVES):
        rows = pl.ds(half * half_rows, half_rows)
        load_half.append(
            [
                load(x_hbm.at[0, 0, :, rows], x_v.at[0, :, rows]),
                load(m_hbm.at[0, rows], m_v.at[rows]),
                load(x_hbm.at[0, 1, :, rows], x_v.at[1, :, rows]),
            ]
        )
    load_sel = load(sel_hbm, sel_v)
    load_back = load(tab_hbm.at[pl.ds(GROUP, GROUP)], back_v)

    def first(axis, d, c):
        part = pl.ds(c * PER_CHUNK, PER_CHUNK)
        to = ((z if axis == 0 else y) + d) % SIDE
        return pltpu.make_async_remote_copy(
            src_ref=(zsend if axis == 0 else ysend).at[to, part],
            dst_ref=(zin if axis == 0 else yin).at[z if axis == 0 else y, part],
            send_sem=r1s.at[axis], recv_sem=r1r.at[axis, c],
            device_id=at(y, to) if axis == 0 else at(to, z), device_id_type=MESH,
        )

    def send_half(half):
        for c in range(CHUNKS):
            if c * HALVES // CHUNKS == half:
                for d in FAR_FIRST:
                    first(0, d, c).start()
        for c in range(CHUNKS):
            for g in range(half * SIDE // HALVES, (half + 1) * SIDE // HALVES):

                @pl.when(y != g)
                def _():
                    first(1, (g - y + SIDE) % SIDE, c).start()

    tn = (((0,), (0,)), ((), ()))
    lane = lax.broadcasted_iota(jnp.int32, (CAP, SPAN), 1)
    ones = jnp.ones((SIDE * CAP, COLS), BF16)
    owner_lane = lax.broadcasted_iota(jnp.int32, (CAP, SIDE * SIDE), 1)
    load_own.wait()
    load_tab.wait()
    table = tab_v[...]
    stack = jnp.concatenate([table] * (SPAN // GROUP), axis=0)
    second_list = own_v[1]
    again = second_list == own_v[0, 0:1, :]
    for j in range(1, CAP):
        again = jnp.logical_or(again, second_list == own_v[0, j : j + 1, :])
    fresh = jnp.where(again, 0.0, DECAY).astype(F32)
    for s in range(STEPS):
        own = own_v[s]
        own = jnp.where(own >= 0, own + (owner_lane % SIDE) * PER_OWNER, -1)
        for g in range(SIDE):
            picks = [
                (own[:, g * SIDE + q : g * SIDE + q + 1] == lane).astype(F32)
                for q in range(SIDE)
            ]
            onehot = jnp.concatenate(picks, axis=0).astype(BF16)
            pick_v[s, g] = onehot
            tsel_v[s, g] = dot(onehot, stack).astype(BF16)
    load_g.wait()

    def rows_of(s, g, p):
        return tsel_v[s, g, p * 4 * CAP : (p + 1) * 4 * CAP, :DEPTH]

    def tile_of(products, base, q):
        side = (q // 2) % 2 * COLS
        top = base + q % 4 * CAP
        return products[q // 4][top : top + CAP, side : side + COLS]

    for half in range(HALVES):
        groups = range(half * SIDE // HALVES, (half + 1) * SIDE // HALVES)
        load_half[half][0].wait()
        load_half[half][1].wait()
        for g in groups:
            rows = pl.ds(g * SPAN, SPAN)
            f_v[0, g] = DECAY * m_v[rows, :] + dot(x_v[0, :, rows], g_v[0], tn)
        load_half[half][2].wait()
        for g in groups:
            rows = pl.ds(g * SPAN, SPAN)
            f_v[1, g] = dot(x_v[1, :, rows], g_v[1], tn)
        for s in range(STEPS):
            for g in groups:
                tables = [
                    jnp.concatenate(
                        [table[:, :DEPTH]] + [rows_of(t, g, p) for t in range(s, STEPS)],
                        axis=0,
                    )
                    for p in range(2)
                ]
                products = pair_products(tables, f_v[s, g])
                f_v[s, g] = blocks_of(products)
                for q in range(SIDE):
                    tile = tile_of(products, GROUP, q)
                    if s == 0:
                        o = g * SIDE + q
                        ext_v[g, q] = fresh[:, o : o + 1] * tile_of(
                            products, GROUP + 4 * CAP, q
                        )
                    else:
                        tile = tile + ext_v[g, q]
                    if (g + q) % 2 == 0:
                        zsend[q, g // 2, s * CAP : (s + 1) * CAP, :] = tile
                    else:
                        ysend[g, q // 2, s * CAP : (s + 1) * CAP, :] = tile
        if half == 0:
            pl.semaphore_wait(barrier, 2 * (SIDE - 1))
        send_half(half)

    zin[z] = zsend[z]
    yin[y] = ysend[y]

    load_sel.wait()
    load_back.wait()
    pick_row = lax.broadcasted_iota(jnp.int32, (COLS, SIDE * SIDE), 0)
    pick_lane = lax.broadcasted_iota(jnp.int32, (COLS, SIDE * SIDE), 1)
    place = (lax.broadcasted_iota(jnp.int32, (COLS, COLS), 0) % PER_OWNER).astype(F32)
    nt = (((1,), (1,)), ((), ()))

    def scatter_table(listed, owner):
        chooser = (pick_lane == owner).astype(F32).astype(BF16)
        wanted = dot(chooser, listed.astype(F32).astype(BF16), nt)
        return (wanted == place).astype(F32).astype(BF16)

    along_z = sel_v[pl.ds(y * SIDE, SIDE)].reshape(COLS, SIDE * SIDE)
    along_y = jnp.concatenate(
        [sel_v[q * SIDE + z].reshape(STEPS * CAP, SIDE * SIDE) for q in range(SIDE)], axis=0
    )
    index = pick_row // PER_OWNER
    table_z = scatter_table(along_z, (2 * index + z % 2) * SIDE + z)
    table_y = scatter_table(along_y, y * SIDE + 2 * index + (y + 1) % 2)

    backward = back_v[...]
    for g in range(SIDE):
        keep = [1.0 - dot(pick_v[s, g], ones, tn) for s in range(STEPS)]
        kept_v[g] = keep[1] * (DECAY * keep[0] * f_v[0, g] + f_v[1, g])
    for g in range(SIDE):
        mom_ref[g * SPAN : (g + 1) * SPAN, :] = blocks_apply(backward, kept_v[g])

    def second(axis, i):
        to = 2 * i + (z % 2 if axis == 0 else (y + 1) % 2)
        return to, pltpu.make_async_remote_copy(
            src_ref=(pz if axis == 0 else py).at[i],
            dst_ref=p2in.at[y if axis == 0 else z],
            send_sem=p2s, recv_sem=p2r,
            device_id=at(to, z) if axis == 0 else at(y, to), device_id_type=MESH,
        )

    def others(ref, send_sem, recv_sem):
        return pltpu.make_async_remote_copy(
            src_ref=ref, dst_ref=ref, send_sem=send_sem, recv_sem=recv_sem,
            device_id=at((y + 1) % SIDE, z), device_id_type=MESH,
        )

    def await_recv(ref, sem):
        others(ref, p2s, sem).wait_recv()

    def await_send(ref, sem):
        others(ref, sem, p2r).wait_send()

    for c in range(CHUNKS):
        part = pl.ds(c * PER_CHUNK, PER_CHUNK)
        for axis in range(2):
            await_recv((zin if axis == 0 else yin).at[pl.ds(0, SIDE - 1), part], r1r.at[axis, c])
        for i in range(c * PER_CHUNK, (c + 1) * PER_CHUNK):
            block = slice(i * PER_OWNER, (i + 1) * PER_OWNER)
            for axis in range(2):
                arrived = (zin if axis == 0 else yin)[:, i].reshape(COLS, COLS)
                table = table_z if axis == 0 else table_y
                (pz if axis == 0 else py)[i] = folded(dot(table[block], split(arrived)))
        for i in range(c * PER_CHUNK, (c + 1) * PER_CHUNK):
            for axis in range(2):
                to, copy = second(axis, i)
                here = y if axis == 0 else z

                @pl.when(to != here)
                def _():
                    copy.start()

                @pl.when(to == here)
                def _():
                    p2in[here] = (pz if axis == 0 else py)[i]

    def done1():
        await_send(zsend.at[pl.ds(0, SIDE - 1)], r1s.at[0])
        await_send(ysend.at[pl.ds(0, SIDE - 1)], r1s.at[1])

    along = y + par * (z - y)
    line = z + par * (y - z)
    mine = along // 2
    await_recv(p2in.at[pl.ds(0, SIDE - 1)], p2r)
    total = p2in[0]
    for k in range(1, SIDE):
        total = total + p2in[k]
    tout[...] = total
    u_v[par, line, mine] = total

    def done2():
        done1()
        await_send(p2in.at[pl.ds(0, SIDE - 1)], p2s)

    def third(d):
        to_y = (y + (1 - par) * d) % SIDE
        to_z = (z + par * d) % SIDE
        return pltpu.make_async_remote_copy(
            src_ref=tout, dst_ref=u_v.at[par, line, mine],
            send_sem=a1s, recv_sem=a1r.at[par, mine],
            device_id=at(to_y, to_z), device_id_type=MESH,
        )

    for d in FAR_FIRST:
        third(d).start()

    def third_arrived(axis, i):
        where = z if axis == 0 else y

        @pl.when(jnp.logical_or(par != axis, mine != i))
        def _():
            await_recv(u_v.at[axis, where, i], a1r.at[axis, i])

    def spread(axis, way, hop, behind, first_block, blocks):
        pos = z if axis == 0 else y
        step = 1 if way == 0 else SIDE - 1
        source = (pos + behind * (SIDE - step)) % SIDE
        to = (pos + hop * step) % SIDE
        block = u_v.at[axis, source, pl.ds(first_block, blocks)]
        slot = 2 * (behind + hop - 1) + way
        return pltpu.make_async_remote_copy(
            src_ref=block, dst_ref=block,
            send_sem=a2s.at[axis], recv_sem=a2r.at[axis, slot, first_block // 2],
            device_id=at(y, to) if axis == 0 else at(to, z), device_id_type=MESH,
        )

    def spread_arrived(axis, way, distance, first_block, blocks):
        pos = z if axis == 0 else y
        step = 1 if way == 0 else SIDE - 1
        source = (pos + distance * (SIDE - step)) % SIDE
        block = u_v.at[axis, source, pl.ds(first_block, blocks)]
        await_recv(block, a2r.at[axis, 2 * (distance - 1) + way, first_block // 2])

    for half in range(2):
        for axis in range(2):
            for i in (2 * half, 2 * half + 1):
                third_arrived(axis, i)
                for way in range(2):
                    spread(axis, way, 2, 0, i, 1).start()
    for axis in range(2):
        for way in range(2):
            spread(axis, way, 1, 0, 0, 4).start()
    for half in range(2):
        for axis in range(2):
            for way in range(2):
                spread_arrived(axis, way, 2, 2 * half, 2)
                if half == way:
                    spread(axis, way, 2, 2, 2 * half, 2).start()
                spread(axis, way, 1, 2, 2 * half, 2).start()
    done2()
    await_send(p2in.at[pl.ds(0, SIDE - 1)], a1s)
    for axis in range(2):
        for way in range(2):
            spread_arrived(axis, way, 1, 0, 4)
    for half in range(2):
        for axis in range(2):
            for way in range(2):
                spread_arrived(axis, way, 3, 2 * half, 2)
                if half == way:
                    spread_arrived(axis, way, 4, 2 * half, 2)
    for axis in range(2):
        await_send(u_v.at[axis, pl.ds(0, SIDE - 1)], a2s.at[axis])


def deliver(u_ref, mom_ref, back_ref, upd_out, mom_out, upd_v, sem):
    momentum = pltpu.make_async_copy(mom_ref, mom_out, sem.at[SIDE])
    momentum.start()
    copies = []
    for g in range(SIDE):
        rows = pl.ds(g * SPAN, SPAN)
        parts = [
            u_ref[0, q, g // 2] if (g + q) % 2 == 0 else u_ref[1, g, q // 2]
            for q in range(SIDE)
        ]
        block = blocks_apply(back_ref[...], jnp.concatenate(parts, axis=0))
        upd_v[rows, :] = block.astype(BF16)
        copies.append(pltpu.make_async_copy(upd_v.at[rows], upd_out.at[rows], sem.at[g]))
        copies[-1].start()
    for copy in copies:
        copy.wait()
    momentum.wait()


def per_device(inputs, grad_out, momentum, select):
    table = jnp.asarray(transform_tables())
    listed = jnp.transpose(select, (0, 1, 3, 2))
    hbm = pl.BlockSpec(memory_space=pl.ANY)
    vmem = pl.BlockSpec(memory_space=pltpu.VMEM)
    operands = [
        pltpu.with_memory_space_constraint(v, pltpu.HBM)
        for v in (inputs, grad_out, momentum, listed, table)
    ]
    outs = (
        jax.ShapeDtypeStruct((ROWS, COLS), BF16),
        jax.ShapeDtypeStruct((ROWS, COLS), F32),
    )
    gathered, new_momentum, back = pl.pallas_call(
        kernel,
        out_shape=(
            jax.ShapeDtypeStruct((2, SIDE, 4, PER_OWNER, COLS), F32),
            outs[1],
            jax.ShapeDtypeStruct((GROUP, SPAN), BF16),
        ),
        in_specs=[hbm] * 5,
        out_specs=(vmem, vmem, vmem),
        scratch_shapes=[
            pltpu.VMEM((STEPS, TOK, ROWS), BF16),
            pltpu.VMEM((STEPS, TOK, COLS), BF16),
            pltpu.VMEM((ROWS, COLS), F32),
            pltpu.VMEM((SIDE * SIDE, STEPS, CAP, SIDE * SIDE), jnp.int32),
            pltpu.VMEM((STEPS, CAP, SIDE * SIDE), jnp.int32),
            pltpu.VMEM((GROUP, SPAN), BF16),
            pltpu.VMEM((STEPS, SIDE, SPAN, COLS), F32),
            pltpu.VMEM((SIDE, SPAN, COLS), F32),
            pltpu.VMEM((STEPS, SIDE, SIDE * CAP, SPAN), BF16),
            pltpu.VMEM((STEPS, SIDE, SIDE * CAP, SPAN), BF16),
            pltpu.VMEM((SIDE, SIDE, CAP, COLS), F32),
            pltpu.VMEM((SIDE, 4, STEPS * CAP, COLS), F32),
            pltpu.VMEM((SIDE, 4, STEPS * CAP, COLS), F32),
            pltpu.VMEM((SIDE, 4, STEPS * CAP, COLS), F32),
            pltpu.VMEM((SIDE, 4, STEPS * CAP, COLS), F32),
            pltpu.VMEM((4, PER_OWNER, COLS), F32),
            pltpu.VMEM((4, PER_OWNER, COLS), F32),
            pltpu.VMEM((SIDE, PER_OWNER, COLS), F32),
            pltpu.VMEM((PER_OWNER, COLS), F32),
            pltpu.SemaphoreType.DMA((5 + 3 * HALVES,)),
            pltpu.SemaphoreType.DMA((2,)),
            pltpu.SemaphoreType.DMA((2, CHUNKS)),
            pltpu.SemaphoreType.DMA,
            pltpu.SemaphoreType.DMA,
            pltpu.SemaphoreType.DMA,
            pltpu.SemaphoreType.DMA((2, 4)),
            pltpu.SemaphoreType.DMA((2,)),
            pltpu.SemaphoreType.DMA((2, 8, 2)),
        ],
        compiler_params=pltpu.CompilerParams(
            collective_id=0, has_side_effects=True, vmem_limit_bytes=40 << 20
        ),
    )(*operands)
    update, new_momentum = pl.pallas_call(
        deliver,
        out_shape=outs,
        in_specs=[vmem] * 3,
        out_specs=(hbm, hbm),
        scratch_shapes=[
            pltpu.VMEM((ROWS, COLS), BF16),
            pltpu.SemaphoreType.DMA((SIDE + 1,)),
        ],
        compiler_params=pltpu.CompilerParams(vmem_limit_bytes=16 << 20),
    )(gathered, new_momentum, back)
    return (update, new_momentum[None])


def solution(mesh):
    return jax.shard_map(
        per_device,
        mesh=mesh,
        in_specs=(
            P("dp", None, None, None),
            P("dp", None, None, "mp"),
            P("dp", None, "mp"),
            P(None, None, None, "mp"),
        ),
        out_specs=(P(None, "mp"), P("dp", None, "mp")),
        check_vma=False,
    )
```

```python
import jax
import jax.numpy as jnp
import numpy as np
from jax import lax
from jax.experimental import pallas as pl
from jax.experimental.pallas import tpu as pltpu
from jax.sharding import PartitionSpec as P

GROUP = 64
DECAY = 0.999
SIDE = 8
PER_OWNER = 32
CAP = 8
STEPS = 2
ROWS = 2048
COLS = 128
TOK = 256
SPAN = 256
BF16 = jnp.bfloat16
F32 = jnp.float32
MESH = pl.DeviceIdType.MESH
FAR_FIRST = (4, 3, 5, 2, 6, 1, 7)
NEAR_EVEN = (0, 2, -2, 4)
NEAR_ODD = (1, -1, 3, -3)


def transform_tables():
    u = np.arange(GROUP)[:, None].astype(np.float64)
    i = np.arange(GROUP)[None, :].astype(np.float64)
    scale = np.where(u == 0, np.sqrt(1.0 / GROUP), np.sqrt(2.0 / GROUP))
    dct = (scale * np.cos(np.pi * (2 * i + 1) * u / (2 * GROUP))).astype(np.float32)

    def parts(table):
        high = table.astype(BF16)
        low = (table - high.astype(np.float32)).astype(BF16)
        return np.concatenate([high, high, low, np.zeros_like(low)], 1)

    return np.concatenate([parts(dct), parts(dct.T)], 0)


def split(x):
    high = x.astype(BF16)
    low = (x - high.astype(F32)).astype(BF16)
    return jnp.concatenate([high, low], axis=1)


def dot(a, b, dims=(((1,), (0,)), ((), ()))):
    return lax.dot_general(a, b, dims, preferred_element_type=F32)


def folded(x):
    return x[:, :COLS] + x[:, COLS:]


def pair_products(tables, x):
    high = x.astype(BF16)
    low = (x - high.astype(F32)).astype(BF16)

    def stacked(b):
        rows = slice(b * GROUP, (b + 1) * GROUP)
        return jnp.concatenate([high[rows], low[rows], high[rows]], axis=0)

    return [
        dot(tables[p], jnp.concatenate([stacked(2 * p), stacked(2 * p + 1)], axis=1))
        for p in range(SPAN // GROUP // 2)
    ]


def blocks_of(products):
    out = []
    for r in products:
        out += [r[:GROUP, :COLS], r[:GROUP, COLS:]]
    return jnp.concatenate(out, axis=0)


def blocks_apply(table, x):
    return blocks_of(pair_products([table[:, :DEPTH]] * 2, x))


DEPTH = 3 * GROUP
CHUNKS = 4
HALVES = 2
PER_CHUNK = 4 // CHUNKS


def kernel(
    x_hbm, g_hbm, m_hbm, sel_hbm, tab_hbm,
    u_v, mom_ref, back_v,
    x_v, g_v, m_v, sel_v, own_v, tab_v, f_v, kept_v, pick_v, tsel_v, ext_v,
    zsend, ysend, zin, yin, pz, py, p2in, tout,
    load_sem, r1s, r1r, p2s, p2r, a1s, a1r, a2s, a2r,
):
    me = lax.axis_index("dp")
    mp = lax.axis_index("mp")
    y = me // SIDE
    z = me % SIDE
    par = (y + z) % 2

    def at(yy, zz):
        return (yy * SIDE + zz, mp)

    barrier = pltpu.get_barrier_semaphore()
    for d in range(1, SIDE):
        pl.semaphore_signal(barrier, inc=1, device_id=at((y + d) % SIDE, z), device_id_type=MESH)
        pl.semaphore_signal(barrier, inc=1, device_id=at(y, (z + d) % SIDE), device_id_type=MESH)

    loads = []

    def load(src, dst):
        copy = pltpu.make_async_copy(src, dst, load_sem.at[len(loads)])
        copy.start()
        loads.append(copy)
        return copy

    half_rows = ROWS // HALVES
    load_own = load(sel_hbm.at[me], own_v)
    load_g = load(g_hbm.at[0], g_v)
    load_tab = load(tab_hbm.at[pl.ds(0, GROUP)], tab_v)
    load_half = []
    for half in range(HALVES):
        rows = pl.ds(half * half_rows, half_rows)
        load_half.append(
            [
                load(x_hbm.at[0, 0, :, rows], x_v.at[0, :, rows]),
                load(m_hbm.at[0, rows], m_v.at[rows]),
                load(x_hbm.at[0, 1, :, rows], x_v.at[1, :, rows]),
            ]
        )
    load_sel = load(sel_hbm, sel_v)
    load_back = load(tab_hbm.at[pl.ds(GROUP, GROUP)], back_v)

    def first(axis, d, c):
        part = pl.ds(c * PER_CHUNK, PER_CHUNK)
        to = ((z if axis == 0 else y) + d) % SIDE
        return pltpu.make_async_remote_copy(
            src_ref=(zsend if axis == 0 else ysend).at[to, part],
            dst_ref=(zin if axis == 0 else yin).at[z if axis == 0 else y, part],
            send_sem=r1s.at[axis], recv_sem=r1r.at[axis, c],
            device_id=at(y, to) if axis == 0 else at(to, z), device_id_type=MESH,
        )

    def send_half(half):
        for c in range(CHUNKS):
            if c * HALVES // CHUNKS == half:
                for d in FAR_FIRST:
                    first(0, d, c).start()
        for c in range(CHUNKS):
            for g in range(half * SIDE // HALVES, (half + 1) * SIDE // HALVES):

                @pl.when(y != g)
                def _():
                    first(1, (g - y + SIDE) % SIDE, c).start()

    tn = (((0,), (0,)), ((), ()))
    lane = lax.broadcasted_iota(jnp.int32, (CAP, SPAN), 1)
    ones = jnp.ones((SIDE * CAP, COLS), BF16)
    owner_lane = lax.broadcasted_iota(jnp.int32, (CAP, SIDE * SIDE), 1)
    load_own.wait()
    load_tab.wait()
    table = tab_v[...]
    stack = jnp.concatenate([table] * (SPAN // GROUP), axis=0)
    second_list = own_v[1]
    again = second_list == own_v[0, 0:1, :]
    for j in range(1, CAP):
        again = jnp.logical_or(again, second_list == own_v[0, j : j + 1, :])
    fresh = jnp.where(again, 0.0, DECAY).astype(F32)
    for s in range(STEPS):
        own = own_v[s]
        own = jnp.where(own >= 0, own + (owner_lane % SIDE) * PER_OWNER, -1)
        for g in range(SIDE):
            picks = [
                (own[:, g * SIDE + q : g * SIDE + q + 1] == lane).astype(F32)
                for q in range(SIDE)
            ]
            onehot = jnp.concatenate(picks, axis=0).astype(BF16)
            pick_v[s, g] = onehot
            tsel_v[s, g] = dot(onehot, stack).astype(BF16)
    load_g.wait()

    def rows_of(s, g, p):
        return tsel_v[s, g, p * 4 * CAP : (p + 1) * 4 * CAP, :DEPTH]

    def tile_of(products, base, q):
        side = (q // 2) % 2 * COLS
        top = base + q % 4 * CAP
        return products[q // 4][top : top + CAP, side : side + COLS]

    for half in range(HALVES):
        groups = range(half * SIDE // HALVES, (half + 1) * SIDE // HALVES)
        load_half[half][0].wait()
        load_half[half][1].wait()
        for g in groups:
            rows = pl.ds(g * SPAN, SPAN)
            f_v[0, g] = DECAY * m_v[rows, :] + dot(x_v[0, :, rows], g_v[0], tn)
        load_half[half][2].wait()
        for g in groups:
            rows = pl.ds(g * SPAN, SPAN)
            f_v[1, g] = dot(x_v[1, :, rows], g_v[1], tn)
        for s in range(STEPS):
            for g in groups:
                tables = [
                    jnp.concatenate(
                        [table[:, :DEPTH]] + [rows_of(t, g, p) for t in range(s, STEPS)],
                        axis=0,
                    )
                    for p in range(2)
                ]
                products = pair_products(tables, f_v[s, g])
                f_v[s, g] = blocks_of(products)
                for q in range(SIDE):
                    tile = tile_of(products, GROUP, q)
                    if s == 0:
                        o = g * SIDE + q
                        ext_v[g, q] = fresh[:, o : o + 1] * tile_of(
                            products, GROUP + 4 * CAP, q
                        )
                    else:
                        tile = tile + ext_v[g, q]
                    if (g + q) % 2 == 0:
                        zsend[q, g // 2, s * CAP : (s + 1) * CAP, :] = tile
                    else:
                        ysend[g, q // 2, s * CAP : (s + 1) * CAP, :] = tile
        if half == 0:
            pl.semaphore_wait(barrier, 2 * (SIDE - 1))
        send_half(half)

    zin[z] = zsend[z]
    yin[y] = ysend[y]

    load_sel.wait()
    load_back.wait()
    pick_row = lax.broadcasted_iota(jnp.int32, (COLS, SIDE * SIDE), 0)
    pick_lane = lax.broadcasted_iota(jnp.int32, (COLS, SIDE * SIDE), 1)
    place = (lax.broadcasted_iota(jnp.int32, (COLS, COLS), 0) % PER_OWNER).astype(F32)
    nt = (((1,), (1,)), ((), ()))

    def scatter_table(listed, owner):
        chooser = (pick_lane == owner).astype(F32).astype(BF16)
        wanted = dot(chooser, listed.astype(F32).astype(BF16), nt)
        return (wanted == place).astype(F32).astype(BF16)

    along_z = sel_v[pl.ds(y * SIDE, SIDE)].reshape(COLS, SIDE * SIDE)
    along_y = jnp.concatenate(
        [sel_v[q * SIDE + z].reshape(STEPS * CAP, SIDE * SIDE) for q in range(SIDE)], axis=0
    )
    index = pick_row // PER_OWNER
    table_z = scatter_table(along_z, (2 * index + z % 2) * SIDE + z)
    table_y = scatter_table(along_y, y * SIDE + 2 * index + (y + 1) % 2)

    backward = back_v[...]
    for g in range(SIDE):
        keep = [1.0 - dot(pick_v[s, g], ones, tn) for s in range(STEPS)]
        kept_v[g] = keep[1] * (DECAY * keep[0] * f_v[0, g] + f_v[1, g])
    for g in range(SIDE):
        mom_ref[g * SPAN : (g + 1) * SPAN, :] = blocks_apply(backward, kept_v[g])

    def second(axis, i):
        to = 2 * i + (z % 2 if axis == 0 else (y + 1) % 2)
        return to, pltpu.make_async_remote_copy(
            src_ref=(pz if axis == 0 else py).at[i],
            dst_ref=p2in.at[y if axis == 0 else z],
            send_sem=p2s, recv_sem=p2r,
            device_id=at(to, z) if axis == 0 else at(y, to), device_id_type=MESH,
        )

    def others(ref, send_sem, recv_sem):
        return pltpu.make_async_remote_copy(
            src_ref=ref, dst_ref=ref, send_sem=send_sem, recv_sem=recv_sem,
            device_id=at((y + 1) % SIDE, z), device_id_type=MESH,
        )

    def await_recv(ref, sem):
        others(ref, p2s, sem).wait_recv()

    def await_send(ref, sem):
        others(ref, sem, p2r).wait_send()

    for c in range(CHUNKS):
        part = pl.ds(c * PER_CHUNK, PER_CHUNK)
        for axis in range(2):
            await_recv((zin if axis == 0 else yin).at[pl.ds(0, SIDE - 1), part], r1r.at[axis, c])
        for i in range(c * PER_CHUNK, (c + 1) * PER_CHUNK):
            block = slice(i * PER_OWNER, (i + 1) * PER_OWNER)
            for axis in range(2):
                arrived = (zin if axis == 0 else yin)[:, i].reshape(COLS, COLS)
                table = table_z if axis == 0 else table_y
                (pz if axis == 0 else py)[i] = folded(dot(table[block], split(arrived)))
        for i in range(c * PER_CHUNK, (c + 1) * PER_CHUNK):
            for axis in range(2):
                to, copy = second(axis, i)
                here = y if axis == 0 else z

                @pl.when(to != here)
                def _():
                    copy.start()

                @pl.when(to == here)
                def _():
                    p2in[here] = (pz if axis == 0 else py)[i]

    def done1():
        await_send(zsend.at[pl.ds(0, SIDE - 1)], r1s.at[0])
        await_send(ysend.at[pl.ds(0, SIDE - 1)], r1s.at[1])

    along = y + par * (z - y)
    line = z + par * (y - z)
    mine = along // 2
    await_recv(p2in.at[pl.ds(0, SIDE - 1)], p2r)
    total = p2in[0]
    for k in range(1, SIDE):
        total = total + p2in[k]
    tout[...] = total
    u_v[par, line, mine] = total

    def done2():
        done1()
        await_send(p2in.at[pl.ds(0, SIDE - 1)], p2s)

    def third(d):
        to_y = (y + (1 - par) * d) % SIDE
        to_z = (z + par * d) % SIDE
        return pltpu.make_async_remote_copy(
            src_ref=tout, dst_ref=u_v.at[par, line, mine],
            send_sem=a1s, recv_sem=a1r.at[par, mine],
            device_id=at(to_y, to_z), device_id_type=MESH,
        )

    for d in FAR_FIRST:
        third(d).start()

    def third_arrived(axis, i):
        where = z if axis == 0 else y

        @pl.when(jnp.logical_or(par != axis, mine != i))
        def _():
            await_recv(u_v.at[axis, where, i], a1r.at[axis, i])

    def spread(axis, way, hop, behind, first_block, blocks):
        pos = z if axis == 0 else y
        step = 1 if way == 0 else SIDE - 1
        source = (pos + behind * (SIDE - step)) % SIDE
        to = (pos + hop * step) % SIDE
        block = u_v.at[axis, source, pl.ds(first_block, blocks)]
        slot = 2 * (behind + hop - 1) + way
        return pltpu.make_async_remote_copy(
            src_ref=block, dst_ref=block,
            send_sem=a2s.at[axis], recv_sem=a2r.at[axis, slot, first_block // 2],
            device_id=at(y, to) if axis == 0 else at(to, z), device_id_type=MESH,
        )

    def spread_arrived(axis, way, distance, first_block, blocks):
        pos = z if axis == 0 else y
        step = 1 if way == 0 else SIDE - 1
        source = (pos + distance * (SIDE - step)) % SIDE
        block = u_v.at[axis, source, pl.ds(first_block, blocks)]
        await_recv(block, a2r.at[axis, 2 * (distance - 1) + way, first_block // 2])

    for half in range(2):
        for i in (2 * half, 2 * half + 1):
            for axis in range(2):
                third_arrived(axis, i)
                for way in range(2):
                    spread(axis, way, 2, 0, i, 1).start()
    for axis in range(2):
        for way in range(2):
            spread(axis, way, 1, 0, 0, 4).start()
    for half in range(2):
        for axis in range(2):
            for way in range(2):
                spread_arrived(axis, way, 2, 2 * half, 2)
                if half == way:
                    spread(axis, way, 2, 2, 2 * half, 2).start()
                spread(axis, way, 1, 2, 2 * half, 2).start()
    done2()
    await_send(p2in.at[pl.ds(0, SIDE - 1)], a1s)
    for axis in range(2):
        for way in range(2):
            spread_arrived(axis, way, 1, 0, 4)
    for half in range(2):
        for axis in range(2):
            for way in range(2):
                spread_arrived(axis, way, 3, 2 * half, 2)
                if half == way:
                    spread_arrived(axis, way, 4, 2 * half, 2)
    for axis in range(2):
        await_send(u_v.at[axis, pl.ds(0, SIDE - 1)], a2s.at[axis])


def deliver(u_ref, mom_ref, back_ref, upd_out, mom_out, upd_v, sem):
    momentum = pltpu.make_async_copy(mom_ref, mom_out, sem.at[SIDE])
    momentum.start()
    copies = []
    for g in range(SIDE):
        rows = pl.ds(g * SPAN, SPAN)
        parts = [
            u_ref[0, q, g // 2] if (g + q) % 2 == 0 else u_ref[1, g, q // 2]
            for q in range(SIDE)
        ]
        block = blocks_apply(back_ref[...], jnp.concatenate(parts, axis=0))
        upd_v[rows, :] = block.astype(BF16)
        copies.append(pltpu.make_async_copy(upd_v.at[rows], upd_out.at[rows], sem.at[g]))
        copies[-1].start()
    for copy in copies:
        copy.wait()
    momentum.wait()


def per_device(inputs, grad_out, momentum, select):
    table = jnp.asarray(transform_tables())
    listed = jnp.transpose(select, (0, 1, 3, 2))
    hbm = pl.BlockSpec(memory_space=pl.ANY)
    vmem = pl.BlockSpec(memory_space=pltpu.VMEM)
    operands = [
        pltpu.with_memory_space_constraint(v, pltpu.HBM)
        for v in (inputs, grad_out, momentum, listed, table)
    ]
    outs = (
        jax.ShapeDtypeStruct((ROWS, COLS), BF16),
        jax.ShapeDtypeStruct((ROWS, COLS), F32),
    )
    gathered, new_momentum, back = pl.pallas_call(
        kernel,
        out_shape=(
            jax.ShapeDtypeStruct((2, SIDE, 4, PER_OWNER, COLS), F32),
            outs[1],
            jax.ShapeDtypeStruct((GROUP, SPAN), BF16),
        ),
        in_specs=[hbm] * 5,
        out_specs=(vmem, vmem, vmem),
        scratch_shapes=[
            pltpu.VMEM((STEPS, TOK, ROWS), BF16),
            pltpu.VMEM((STEPS, TOK, COLS), BF16),
            pltpu.VMEM((ROWS, COLS), F32),
            pltpu.VMEM((SIDE * SIDE, STEPS, CAP, SIDE * SIDE), jnp.int32),
            pltpu.VMEM((STEPS, CAP, SIDE * SIDE), jnp.int32),
            pltpu.VMEM((GROUP, SPAN), BF16),
            pltpu.VMEM((STEPS, SIDE, SPAN, COLS), F32),
            pltpu.VMEM((SIDE, SPAN, COLS), F32),
            pltpu.VMEM((STEPS, SIDE, SIDE * CAP, SPAN), BF16),
            pltpu.VMEM((STEPS, SIDE, SIDE * CAP, SPAN), BF16),
            pltpu.VMEM((SIDE, SIDE, CAP, COLS), F32),
            pltpu.VMEM((SIDE, 4, STEPS * CAP, COLS), F32),
            pltpu.VMEM((SIDE, 4, STEPS * CAP, COLS), F32),
            pltpu.VMEM((SIDE, 4, STEPS * CAP, COLS), F32),
            pltpu.VMEM((SIDE, 4, STEPS * CAP, COLS), F32),
            pltpu.VMEM((4, PER_OWNER, COLS), F32),
            pltpu.VMEM((4, PER_OWNER, COLS), F32),
            pltpu.VMEM((SIDE, PER_OWNER, COLS), F32),
            pltpu.VMEM((PER_OWNER, COLS), F32),
            pltpu.SemaphoreType.DMA((5 + 3 * HALVES,)),
            pltpu.SemaphoreType.DMA((2,)),
            pltpu.SemaphoreType.DMA((2, CHUNKS)),
            pltpu.SemaphoreType.DMA,
            pltpu.SemaphoreType.DMA,
            pltpu.SemaphoreType.DMA,
            pltpu.SemaphoreType.DMA((2, 4)),
            pltpu.SemaphoreType.DMA((2,)),
            pltpu.SemaphoreType.DMA((2, 8, 2)),
        ],
        compiler_params=pltpu.CompilerParams(
            collective_id=0, has_side_effects=True, vmem_limit_bytes=40 << 20
        ),
    )(*operands)
    update, new_momentum = pl.pallas_call(
        deliver,
        out_shape=outs,
        in_specs=[vmem] * 3,
        out_specs=(hbm, hbm),
        scratch_shapes=[
            pltpu.VMEM((ROWS, COLS), BF16),
            pltpu.SemaphoreType.DMA((SIDE + 1,)),
        ],
        compiler_params=pltpu.CompilerParams(vmem_limit_bytes=16 << 20),
    )(gathered, new_momentum, back)
    return (update, new_momentum[None])


def solution(mesh):
    return jax.shard_map(
        per_device,
        mesh=mesh,
        in_specs=(
            P("dp", None, None, None),
            P("dp", None, None, "mp"),
            P("dp", None, "mp"),
            P(None, None, None, "mp"),
        ),
        out_specs=(P(None, "mp"), P("dp", None, "mp")),
        check_vma=False,
    )
```
